128 devices in a mesh: trade: 16 (over y, x), path: 8 (over z, core).
Axes of the slice: x: 4, y: 4, z: 4, core: 2. Of those that a mesh axis runs over, the one named last changes fastest.
Arguments:
- deltas: bfloat16 [65536, 1024], P('trade', 'path'), may hold values from -0.0039978027 to 0.0039978027
- net_ids: int32 [65536], P('trade'), may hold values from 0 to 7, as said below
- block_ids: int32 [65536], P('trade'), may hold values from 0 to 13823
- bucket_map: int32 [13824], replicated, may hold values from 0 to 1151
- risk_weight: float32 [13824], replicated, may hold values from 10 to 80
- counts: int32 [16], P('trade'), may hold values from 1 to 4096, 39321 in all
- correlation: float32 [1152, 1152], replicated, may hold values from -1 to 3, as said below
- path_weight: float32 [1024], P('path'), may hold values from 0.2 to 16.2, as said below
- margin_cotangent: float32 [8, 1024], P(None, 'path'), may hold values from -6 to 6
Outputs:
- margin: float32 [8, 1024], P(None, 'path')
- expected: float32 [8], replicated
- trade_grad: bfloat16 [65536, 1024], P('trade', 'path')
The draws below stay inside these ranges and needn't reach their ends.
Inputs may be any that keep to these rules, and one draw needn't show every extreme that they name: The live trades of group g fill its first counts[g] of 4096 slots; some group is full. `net_ids`: among the 4096 slots of one trade group each netting set appears at most 768 times, and in every group one netting set appears exactly 768 times. `correlation`: symmetric and positive definite. `path_weight`: Positive.
All inputs are finite; a program needn't handle non-finite values.
Results may differ from the reference program's by a relative error of at most 0.0054.
The reference program's roundings to bfloat16 on the way (of `weighted` and `bucket_grad`) count: a program that leaves them out, or rounds other values in their place, can miss the bound.
Values may be sent and summed in bfloat16 or wider, within the bound.
A program may use at most 64 MiB of HBM per device.

```python
import math
import jax
import jax.numpy as jnp
import numpy as np
from jax import lax

BUCKETS = 1152
TENOR_BLOCKS = 13824
NETS = 8
TRADE_CAP = 4096
MOST = 768
GROUPS = 16
TRADES = 65536
PATHS = 1024
N_TRADE = 16


def draw_net_ids(key, part):
    group_total = TRADES // TRADE_CAP
    pool_size = NETS * MOST
    pool = (jnp.arange(pool_size, dtype=jnp.int32) // MOST).astype(jnp.int32)
    base_key = jax.random.fold_in(key, 31)

    def one_group(group):
        group_key = jax.random.fold_in(base_key, group)
        first_key = jax.random.fold_in(group_key, 1)
        second_key = jax.random.fold_in(group_key, 2)
        third_key = jax.random.fold_in(group_key, 3)
        special = jax.random.randint(first_key, (), 0, NETS, dtype=jnp.int32)
        order = jax.random.permutation(second_key, pool_size).astype(jnp.int32)
        score = jnp.where(pool == special, order - pool_size, order).astype(jnp.int32)
        picked = pool[jnp.argsort(score, stable=True)[:TRADE_CAP]]
        shuffle = jax.random.permutation(third_key, TRADE_CAP).astype(jnp.int32)
        return picked[shuffle]
    return lax.map(one_group, jnp.arange(group_total, dtype=jnp.int32)).reshape(TRADES).astype(jnp.int32)


def draw_correlation(key, part):
    factor_key = jax.random.fold_in(key, 11)
    factor = jax.random.normal(factor_key, (BUCKETS, BUCKETS), jnp.float32)
    product = jnp.dot(factor, factor.T, precision=lax.Precision.HIGHEST) / BUCKETS
    return 0.5 * (product + product.T) + 0.5 * jnp.eye(BUCKETS, dtype=jnp.float32)


def draw_path_weight(key, part):
    jitter_key = jax.random.fold_in(key, 23)
    position = jnp.arange(PATHS, dtype=jnp.float32) / max(PATHS - 1, 1)
    rising = 1.0 + 2.0 * position
    jitter = jax.random.uniform(jitter_key, (PATHS,), jnp.float32, 0.5, 1.5)
    return rising * jitter


def set_ends(entries, key, smallest, largest):
    shape = entries.shape
    spot = [jax.random.randint(jax.random.fold_in(key, axis), (), 0, shape[axis]) for axis in range(len(shape))]
    entries = entries.at[tuple(spot)].set(smallest)
    longest = shape.index(max(shape))
    spot[longest] = (spot[longest] + 1) % shape[longest]
    return entries.at[tuple(spot)].set(largest)


def block_levels(rng, shape, cuts, low, largest):
    loudness, own = 1.0, jax.random.fold_in(rng, 6)
    for dim, shards_of in cuts:
        heights = jnp.exp(jax.random.uniform(jax.random.fold_in(own, dim), (shards_of,), jnp.float32, low / len(cuts), largest / len(cuts)))
        loudness = loudness * jnp.repeat(heights, shape[dim] // shards_of).reshape([-1 if axis == dim else 1 for axis in range(len(shape))])
    return loudness


def split_up(amount, total, most, slope):
    portions = [(1 << 20) // math.isqrt(grade ** slope) + 1 for grade in range(2, amount + 1)]
    rest, given = total - most - (amount - 1), [1] * (amount - 1)
    while rest > 0:
        candidates = [i for i in range(amount - 1) if given[i] < most]
        whole, left = sum([portions[i] for i in candidates]), rest
        for i in candidates:
            extra = min(most - given[i], max(1, left * portions[i] // whole), rest)
            given[i] = given[i] + extra
            rest = rest - extra
    return np.array([most] + given)


def ragged_sizes(stream_key, amount, total, reach, lean):
    if amount == 2:
        one = jax.random.randint(stream_key, (), max(1, total - reach), min(reach, total - 1) + 1)
        return jnp.stack([one, total - one])
    sizes = jnp.asarray(split_up(amount, total, reach, lean), jnp.int32)
    couples = (amount - 1) // 2
    source_of, receiver = sizes[1:1 + 2 * couples:2], sizes[2:2 + 2 * couples:2]
    slack = jnp.minimum(source_of - 1, reach - receiver)
    shifted = jax.random.randint(jax.random.fold_in(stream_key, 1), (couples,), 0, 1 << 20) % (slack + 1)
    sizes = sizes.at[1:1 + 2 * couples:2].set(source_of - shifted).at[2:2 + 2 * couples:2].set(receiver + shifted)
    return sizes[jax.random.permutation(jax.random.fold_in(stream_key, 2), amount)]


def centred(rng, shape, spread, most, cuts=(), kind=jnp.bfloat16):
    loudness = block_levels(rng, shape, cuts, -0.22, 0.18) if cuts else 1.0
    values = jax.random.normal(rng, shape, jnp.float32) * spread * loudness
    return jnp.minimum(jnp.maximum(values, -most), most).astype(kind)


def setup_inputs(seed: int = 0) -> dict:
    arg_keys = jax.random.split(jax.random.key(seed), 10)
    return {
        "deltas": centred(arg_keys[0], (TRADES, PATHS), 0.0005, 0.0039978027, ((0, 16), (1, 8))),
        "net_ids": draw_net_ids(jax.random.fold_in(arg_keys[9], 71), 0),
        "block_ids": set_ends(jax.random.randint(arg_keys[2], (TRADES,), 0, TENOR_BLOCKS), jax.random.fold_in(arg_keys[2], 1), 0, TENOR_BLOCKS - 1).astype(jnp.int32),
        "bucket_map": set_ends(jax.random.randint(arg_keys[3], (TENOR_BLOCKS,), 0, BUCKETS), jax.random.fold_in(arg_keys[3], 1), 0, BUCKETS - 1).astype(jnp.int32),
        "risk_weight": jnp.clip(jnp.exp(jax.random.uniform(arg_keys[4], (TENOR_BLOCKS,), jnp.float32, math.log(10.0), math.log(80.0))), 10.0, 80.0),
        "counts": ragged_sizes(arg_keys[5], GROUPS, TRADE_CAP * N_TRADE * 3 // 5, TRADE_CAP, 2).astype(jnp.int32),
        "correlation": draw_correlation(jax.random.fold_in(arg_keys[9], 71), 0),
        "path_weight": draw_path_weight(jax.random.fold_in(arg_keys[9], 71), 0),
        "margin_cotangent": centred(arg_keys[8], (NETS, PATHS), 1.0, 6.0, ((1, 8),), jnp.float32),
    }


EPSILON = 1e-06

def reference(deltas, net_ids, block_ids, bucket_map, risk_weight, counts, correlation, path_weight, margin_cotangent):
    total_slots = deltas.shape[0]
    path_total = deltas.shape[1]
    position = jnp.arange(total_slots, dtype=jnp.int32)
    group_of = (position // TRADE_CAP).astype(jnp.int32)
    slot_of = (position % TRADE_CAP).astype(jnp.int32)
    is_live = slot_of < counts[group_of]
    trade_weight = risk_weight[block_ids]
    trade_bucket = bucket_map[block_ids]
    weighted = jnp.where(is_live[:, None], trade_weight[:, None] * deltas.astype(jnp.float32), 0.0).astype(jnp.bfloat16)
    segment_key = (trade_bucket * NETS + net_ids).astype(jnp.int32)
    summed = jax.ops.segment_sum(weighted.astype(jnp.float32), segment_key, num_segments=BUCKETS * NETS)
    summed = summed.reshape(BUCKETS, NETS * path_total)
    coupled = jnp.dot(correlation, summed, precision=lax.Precision.HIGHEST, preferred_element_type=jnp.float32)
    quad_form = lax.optimization_barrier(jnp.sum(summed * coupled, axis=0))
    margin_flat = jnp.sqrt(quad_form + EPSILON)
    margin = margin_flat.reshape(NETS, path_total)
    expected = lax.optimization_barrier(jnp.sum(margin * path_weight[None, :], axis=1)) / PATHS
    bucket_grad = ((margin_cotangent.reshape(NETS * path_total) / margin_flat)[None, :] * coupled).astype(jnp.bfloat16)
    bucket_grad = bucket_grad.reshape(BUCKETS, NETS, path_total)
    chosen = bucket_grad[trade_bucket, net_ids]
    trade_grad = jnp.where(is_live[:, None], trade_weight[:, None] * chosen.astype(jnp.float32), 0.0).astype(jnp.bfloat16)
    return (margin, expected, trade_grad)
```

```python
import functools

import jax
import jax.numpy as jnp
from jax import lax
from jax.experimental import pallas as pl
from jax.experimental.pallas import tpu as pltpu
from jax.sharding import PartitionSpec as P

EPSILON = 1e-06
LANES = 128
F32 = jnp.float32
BF16 = jnp.bfloat16
MESH = pl.DeviceIdType.MESH
SIDE = 4
OTHERS = SIDE - 1
CHUNK = 512
NT = (((1,), (1,)), ((), ()))
NN = (((1,), (0,)), ((), ()))
TN = (((0,), (0,)), ((), ()))


def dot(a, b, dims):
    return lax.dot_general(a, b, dims, preferred_element_type=F32)


def tiles_of(total):
    cuts, at = [], 0
    while at < total:
        width = min(256, total - at)
        cuts.append((at, width))
        at += width
    return cuts


def kernel(
    groups,
    slabs,
    deltas,
    nets,
    blocks,
    rw,
    bm,
    counts,
    corr,
    pw,
    cot,
    margin_o,
    expected_o,
    grad_o,
    table,
    hot,
    X,
    wrow,
    S,
    recv1,
    st,
    recv2,
    SF,
    C,
    Chi,
    Clo,
    G,
    acc,
    m_send,
    m_recv,
    e_send,
    e_recv,
    c_sem,
    s_sems,
    r_sems,
    ms_sems,
    mr_sems,
    es_sems,
    er_sems,
):
    me = lax.axis_index("trade")
    slab = lax.axis_index("path")
    y, x = me // SIDE, me % SIDE
    capacity = deltas.shape[0]
    bucket_count = corr.shape[0]
    net_count, paths = cot.shape
    rows = net_count * paths
    own_rows = rows // groups
    tiles = tiles_of(bucket_count)

    barrier = pltpu.get_barrier_semaphore()
    for d in range(1, groups):
        pl.semaphore_signal(barrier, inc=1, device_id={"trade": (me + d) % groups}, device_id_type=MESH)
    for d in range(1, slabs):
        pl.semaphore_signal(barrier, inc=1, device_id={"path": (slab + d) % slabs}, device_id_type=MESH)

    c_copy = pltpu.make_async_copy(corr, C, c_sem)
    c_copy.start()

    table_rows = rw.shape[0]
    table[...] = jnp.zeros_like(table)
    w_all = rw[...]
    w1 = w_all.astype(BF16)
    w2 = (w_all - w1.astype(F32)).astype(BF16)
    b_all = bm[...]
    table[0:table_rows, 0:LANES] = w1
    table[0:table_rows, LANES : 2 * LANES] = w2
    table[0:table_rows, 2 * LANES : 3 * LANES] = (b_all // LANES).astype(F32).astype(BF16)
    table[0:table_rows, 3 * LANES : 4 * LANES] = (b_all % LANES).astype(F32).astype(BF16)
    live_count = counts[0]

    def look_up(i, carry):
        at = pl.multiple_of(i * CHUNK, CHUNK)
        ids = blocks[:, pl.ds(at, CHUNK)]
        high, low = ids // LANES, ids % LANES
        sub = lax.broadcasted_iota(jnp.int32, (LANES, CHUNK), 0)
        pick = jnp.where(sub == high, 1.0, 0.0).astype(BF16)
        found = dot(table[...], pick, TN)
        keep = sub == low
        parts = [
            jnp.sum(jnp.where(keep, found[k * LANES : (k + 1) * LANES], 0.0), axis=0, keepdims=True)
            for k in range(4)
        ]
        slot = at + lax.broadcasted_iota(jnp.int32, (1, CHUNK), 1)
        w = jnp.where(slot < live_count, parts[0] + parts[1], 0.0)
        wrow[0:1, pl.ds(at, CHUNK)] = w
        wrow[1:2, pl.ds(at, CHUNK)] = parts[2] * LANES + parts[3]
        turned = deltas[pl.ds(at, CHUNK), :].astype(F32).T
        weighted = (turned * w).astype(BF16)
        net = nets[:, pl.ds(at, CHUNK)]
        for n in range(net_count):
            mask = jnp.where(net == n, 1.0, 0.0).astype(BF16)
            X[n * paths : (n + 1) * paths, pl.ds(at, CHUNK)] = weighted * mask
        return carry

    lax.fori_loop(0, capacity // CHUNK, look_up, 0)

    def send(src, dst, phase, tile, d, peer):
        copy = pltpu.make_async_remote_copy(
            src_ref=src,
            dst_ref=dst,
            send_sem=s_sems.at[phase, tile, d - 1],
            recv_sem=r_sems.at[phase, tile, d - 1],
            device_id={"trade": peer},
            device_id_type=MESH,
        )
        copy.start()
        return copy

    def row_mate(d):
        return (x + d) % SIDE

    def column_mate(d):
        return (y + d) % SIDE

    def first_stage(t):
        at, width = tiles[t]
        cols = pl.ds(at, width)
        copies = []
        for d in (2, 1, 3):
            kx, ky = row_mate(d), column_mate(d)
            copies.append(send(S.at[:, kx, 0, :, cols], recv1.at[0, d - 1, :, :, cols], 0, t, d, y * SIDE + kx))
            copies.append(send(S.at[ky, :, 1, :, cols], recv1.at[1, d - 1, :, :, cols], 1, t, d, ky * SIDE + x))
        return copies

    def second_stage(t, arriving):
        at, width = tiles[t]
        cols = pl.ds(at, width)
        for copy in arriving:
            copy.wait_recv()
        total_a = S[:, x, 0, :, cols].astype(F32)
        total_b = S[y, :, 1, :, cols].astype(F32)
        for d in range(OTHERS):
            total_a += recv1[0, d, :, :, cols].astype(F32)
            total_b += recv1[1, d, :, :, cols].astype(F32)
        st[0, :, :, cols] = total_a.astype(BF16)
        st[1, :, :, cols] = total_b.astype(BF16)
        copies = []
        for d in (2, 1, 3):
            kx, ky = row_mate(d), column_mate(d)
            copies.append(send(st.at[0, ky, :, cols], recv2.at[0, d - 1, :, cols], 2, t, d, ky * SIDE + x))
            copies.append(send(st.at[1, kx, :, cols], recv2.at[1, d - 1, :, cols], 3, t, d, y * SIDE + kx))
        return copies

    def forward(t):
        at, width = tiles[t]
        for i in range(capacity // CHUNK):
            part = pl.ds(i * CHUNK, CHUNK)
            bucket = wrow[1:2, part]
            sub = (at + lax.broadcasted_iota(jnp.int32, (width, CHUNK), 0)).astype(F32)
            hot[at : at + width, part] = jnp.where(sub == bucket, 1.0, 0.0).astype(BF16)
        result = dot(X[...], hot[at : at + width, :], NT)
        S[:, :, :, :, at : at + width] = result.astype(BF16).reshape(S.shape[:-1] + (width,))

    sent = []
    stage1, stage2 = [], []
    for t in range(len(tiles)):
        forward(t)
        if t == 0:
            pl.semaphore_wait(barrier, groups - 1 + slabs - 1)
        stage1.append(first_stage(t))
        if t >= 1:
            stage2.append(second_stage(t - 1, stage1[t - 1]))
    c_copy.wait()
    for at, width in tiles:
        block = C[:, at : at + width]
        high = block.astype(BF16)
        Chi[:, at : at + width] = high
        Clo[:, at : at + width] = (block - high.astype(F32)).astype(BF16)
    stage2.append(second_stage(len(tiles) - 1, stage1[-1]))
    for t, (at, width) in enumerate(tiles):
        for copy in stage2[t]:
            copy.wait_recv()
        cols = pl.ds(at, width)
        total_a = st[0, y, :, cols].astype(F32)
        total_b = st[1, x, :, cols].astype(F32)
        for d in range(OTHERS):
            total_a += recv2[0, d, :, cols].astype(F32)
            total_b += recv2[1, d, :, cols].astype(F32)
        SF[0 : own_rows // 2, cols] = total_a
        SF[own_rows // 2 : own_rows, cols] = total_b

    summed = SF[...]
    s_high = summed.astype(BF16)
    s_low = (summed - s_high.astype(F32)).astype(BF16)
    both = dot(jnp.concatenate([s_high, s_low], axis=0), Chi[...], NN)
    coupled = both[0:own_rows] + both[own_rows:] + dot(s_high, Clo[...], NN)
    margin = jnp.sqrt(jnp.sum(summed * coupled, axis=1, keepdims=True) + EPSILON)
    per_net = paths // own_rows
    own_net, own_part = me // per_net, me % per_net
    sub = lax.broadcasted_iota(jnp.int32, (own_rows, paths), 0)
    lane = lax.broadcasted_iota(jnp.int32, (own_rows, paths), 1)
    mine = lane == sub + own_part * own_rows
    net_sub = lax.broadcasted_iota(jnp.int32, (net_count, paths), 0)
    cot_row = jnp.sum(jnp.where(net_sub == own_net, cot[...], 0.0), axis=0, keepdims=True)
    cot_column = jnp.sum(jnp.where(mine, cot_row, 0.0), axis=1, keepdims=True)
    grad = ((cot_column / margin) * coupled).astype(BF16)
    G[y, x] = grad.reshape(2, own_rows // 2, bucket_count)

    gather1, gather2 = [], []
    for t, (at, width) in enumerate(tiles):
        cols = pl.ds(at, width)
        copies = []
        for d in (2, 1, 3):
            kx, ky = row_mate(d), column_mate(d)
            own_a, own_b = G.at[y, x, 0, :, cols], G.at[y, x, 1, :, cols]
            copies.append(send(own_a, own_a, 4, t, d, ky * SIDE + x))
            copies.append(send(own_b, own_b, 5, t, d, y * SIDE + kx))
        gather1.append(copies)

    margin_row = jnp.sum(jnp.where(mine, margin, 0.0), axis=0, keepdims=True)
    my_margins = jnp.where(net_sub == own_net, margin_row, 0.0)
    m_send[...] = my_margins
    m_copies = []
    for d in range(1, groups):
        copy = pltpu.make_async_remote_copy(
            src_ref=m_send,
            dst_ref=m_recv.at[d - 1],
            send_sem=ms_sems.at[d - 1],
            recv_sem=mr_sems.at[d - 1],
            device_id={"trade": (me + d) % groups},
            device_id_type=MESH,
        )
        copy.start()
        m_copies.append(copy)

    def gather_second(t):
        at, width = tiles[t]
        cols = pl.ds(at, width)
        for copy in gather1[t]:
            copy.wait_recv()
        copies = []
        for d in (2, 1, 3):
            kx, ky = row_mate(d), column_mate(d)
            all_a, all_b = G.at[:, x, 0, :, cols], G.at[y, :, 1, :, cols]
            copies.append(send(all_a, all_a, 6, t, d, y * SIDE + kx))
            copies.append(send(all_b, all_b, 7, t, d, ky * SIDE + x))
        return copies

    def backward(t):
        at, width = tiles[t]
        step = 256

        def one(i, carry):
            start = pl.multiple_of(i * step, step)
            part = pl.ds(start, step)
            all_grad = G[:, :, :, :, at : at + width].reshape(rows, width)
            looked_up = dot(all_grad, hot[at : at + width, part], NN)
            net = nets[:, part]
            total = jnp.zeros((paths, step), F32) if t == 0 else acc[:, part]
            for n in range(net_count):
                total += jnp.where(net == n, looked_up[n * paths : (n + 1) * paths], 0.0)
            acc[:, part] = total
            return carry

        lax.fori_loop(0, capacity // step, one, 0)

    e_copies = []
    for t in range(len(tiles)):
        gather2.append(gather_second(t))
    for copy in m_copies:
        copy.wait_recv()
    all_margins = my_margins
    for d in range(groups - 1):
        all_margins += m_recv[d]
    margin_o[...] = all_margins
    my_sum = jnp.sum(all_margins * pw[...], axis=1, keepdims=True)
    e_send[...] = jnp.broadcast_to(my_sum, e_send.shape)
    for d in range(1, slabs):
        copy = pltpu.make_async_remote_copy(
            src_ref=e_send,
            dst_ref=e_recv.at[d - 1],
            send_sem=es_sems.at[d - 1],
            recv_sem=er_sems.at[d - 1],
            device_id={"path": (slab + d) % slabs},
            device_id_type=MESH,
        )
        copy.start()
        e_copies.append(copy)

    for t in range(len(tiles)):
        for copy in gather2[t]:
            copy.wait_recv()
        backward(t)

    def finish(i, carry):
        at = pl.multiple_of(i * CHUNK, CHUNK)
        part = pl.ds(at, CHUNK)
        scaled = acc[:, part] * wrow[0:1, part]
        grad_o[part, :] = scaled.T.astype(BF16)
        return carry

    lax.fori_loop(0, capacity // CHUNK, finish, 0)

    for copy in e_copies:
        copy.wait_recv()
    everyone = e_send[...]
    for d in range(slabs - 1):
        everyone += e_recv[d]
    expected_o[...] = everyone / (paths * slabs)

    for group in stage1 + stage2 + gather1 + gather2:
        for copy in group:
            copy.wait_send()
    for copy in m_copies + e_copies:
        copy.wait_send()


def shards(groups, slabs, deltas, net_ids, block_ids, bucket_map, risk_weight, counts, correlation, path_weight, margin_cotangent):
    capacity, paths = deltas.shape
    buckets = correlation.shape[0]
    net_count = margin_cotangent.shape[0]
    rows = net_count * paths
    half = rows // groups // 2
    tile_count = len(tiles_of(buckets))
    vmem = pl.BlockSpec(memory_space=pltpu.VMEM)
    smem = pl.BlockSpec(memory_space=pltpu.SMEM)
    dma = pltpu.SemaphoreType.DMA
    margin, expected, trade_grad = pl.pallas_call(
        functools.partial(kernel, groups, slabs),
        out_shape=(
            jax.ShapeDtypeStruct((net_count, paths), F32),
            jax.ShapeDtypeStruct((net_count, paths), F32),
            jax.ShapeDtypeStruct((capacity, paths), BF16),
        ),
        in_specs=[vmem, vmem, vmem, vmem, vmem, smem, pl.BlockSpec(memory_space=pl.ANY), vmem, vmem],
        out_specs=(vmem, vmem, vmem),
        scratch_shapes=[
            pltpu.VMEM((LANES, 4 * LANES), BF16),
            pltpu.VMEM((buckets, capacity), BF16),
            pltpu.VMEM((rows, capacity), BF16),
            pltpu.VMEM((2, capacity), F32),
            pltpu.VMEM((SIDE, SIDE, 2, half, buckets), BF16),
            pltpu.VMEM((2, OTHERS, SIDE, half, buckets), BF16),
            pltpu.VMEM((2, SIDE, half, buckets), BF16),
            pltpu.VMEM((2, OTHERS, half, buckets), BF16),
            pltpu.VMEM((2 * half, buckets), F32),
            pltpu.VMEM((buckets, buckets), F32),
            pltpu.VMEM((buckets, buckets), BF16),
            pltpu.VMEM((buckets, buckets), BF16),
            pltpu.VMEM((SIDE, SIDE, 2, half, buckets), BF16),
            pltpu.VMEM((paths, capacity), F32),
            pltpu.VMEM((net_count, paths), F32),
            pltpu.VMEM((groups - 1, net_count, paths), F32),
            pltpu.VMEM((net_count, paths), F32),
            pltpu.VMEM((slabs - 1, net_count, paths), F32),
            dma,
            dma((8, tile_count, OTHERS)),
            dma((8, tile_count, OTHERS)),
            dma((groups - 1,)),
            dma((groups - 1,)),
            dma((slabs - 1,)),
            dma((slabs - 1,)),
        ],
        compiler_params=pltpu.CompilerParams(
            collective_id=0, has_side_effects=True, vmem_limit_bytes=60 * 1024 * 1024
        ),
        name="margin_exchange",
    )(
        deltas,
        net_ids.reshape(1, capacity),
        block_ids.reshape(1, capacity),
        risk_weight.reshape(-1, LANES),
        bucket_map.reshape(-1, LANES),
        counts,
        correlation,
        path_weight.reshape(1, paths),
        margin_cotangent,
    )
    return margin, expected[:, 0], trade_grad


def solution(mesh):
    placed = (
        P("trade", "path"),
        P("trade"),
        P("trade"),
        P(),
        P(),
        P("trade"),
        P(),
        P("path"),
        P(None, "path"),
    )
    return jax.shard_map(
        functools.partial(shards, mesh.shape["trade"], mesh.shape["path"]),
        mesh=mesh,
        in_specs=placed,
        out_specs=(P(None, "path"), P(), P("trade", "path")),
        check_vma=False,
    )
```

```python
import functools

import jax
import jax.numpy as jnp
from jax import lax
from jax.experimental import pallas as pl
from jax.experimental.pallas import tpu as pltpu
from jax.sharding import PartitionSpec as P

EPSILON = 1e-06
LANES = 128
F32 = jnp.float32
BF16 = jnp.bfloat16
MESH = pl.DeviceIdType.MESH
SIDE = 4
OTHERS = SIDE - 1
CHUNK = 512
NT = (((1,), (1,)), ((), ()))
NN = (((1,), (0,)), ((), ()))
TN = (((0,), (0,)), ((), ()))


def dot(a, b, dims):
    return lax.dot_general(a, b, dims, preferred_element_type=F32)


TILE = 256


def tiles_of(total):
    cuts, at = [], 0
    while at < total:
        width = min(TILE, total - at)
        cuts.append((at, width))
        at += width
    return cuts


def kernel(
    groups,
    slabs,
    deltas,
    nets,
    blocks,
    rw,
    bm,
    counts,
    corr,
    pw,
    cot,
    margin_o,
    expected_o,
    weight_o,
    chosen_o,
    slots,
    table,
    hot,
    X,
    wrow,
    S,
    recv1,
    st,
    recv2,
    SF,
    C,
    Chi,
    Clo,
    G,
    acc,
    m_send,
    m_recv,
    e_send,
    e_recv,
    c_sem,
    d_sem,
    s_sems,
    r_sems,
    ms_sems,
    mr_sems,
    es_sems,
    er_sems,
):
    me = lax.axis_index("trade")
    slab = lax.axis_index("path")
    y, x = me // SIDE, me % SIDE
    capacity = deltas.shape[0]
    bucket_count = corr.shape[0]
    net_count, paths = cot.shape
    rows = net_count * paths
    own_rows = rows // groups
    tiles = tiles_of(bucket_count)

    barrier = pltpu.get_barrier_semaphore()
    for d in range(1, groups):
        pl.semaphore_signal(barrier, inc=1, device_id={"trade": (me + d) % groups}, device_id_type=MESH)
    for d in range(1, slabs):
        pl.semaphore_signal(barrier, inc=1, device_id={"path": (slab + d) % slabs}, device_id_type=MESH)

    d_copy = pltpu.make_async_copy(deltas, slots, d_sem)
    d_copy.start()
    c_copy = pltpu.make_async_copy(corr, C, c_sem)
    c_copy.start()

    table_rows = rw.shape[0]
    w_all = rw[...]
    w1 = w_all.astype(BF16).astype(F32)
    b_all = bm[...]
    parts = (w1, w_all - w1, (b_all // LANES).astype(F32), (b_all % LANES).astype(F32))
    table[...] = jnp.zeros_like(table)
    for k, part in enumerate(parts):
        table[k * LANES : (k + 1) * LANES, 0:table_rows] = part.T.astype(BF16)
    live_count = counts[0]
    acc[...] = jnp.zeros_like(acc)
    padded = hot.shape[0]
    if padded > bucket_count:
        G[:, :, :, :, bucket_count:padded] = jnp.zeros(G.shape[:-1] + (padded - bucket_count,), BF16)
    d_copy.wait()

    def look_up(i, carry):
        at = pl.multiple_of(i * CHUNK, CHUNK)
        ids = blocks[:, pl.ds(at, CHUNK)]
        high, low = ids // LANES, ids % LANES
        sub = lax.broadcasted_iota(jnp.int32, (LANES, CHUNK), 0)
        pick = jnp.where(sub == high, 1.0, 0.0).astype(BF16)
        found = dot(table[...], pick, NN)
        keep = sub == low
        parts = [
            jnp.sum(jnp.where(keep, found[k * LANES : (k + 1) * LANES], 0.0), axis=0, keepdims=True)
            for k in range(4)
        ]
        slot = at + lax.broadcasted_iota(jnp.int32, (1, CHUNK), 1)
        w = jnp.where(slot < live_count, parts[0] + parts[1], 0.0)
        weight_o[:, pl.ds(at, CHUNK)] = w
        wrow[:, pl.ds(at, CHUNK)] = parts[2] * LANES + parts[3]
        turned = slots[pl.ds(at, CHUNK), :].astype(F32).T
        weighted = (turned * w).astype(BF16)
        net = nets[:, pl.ds(at, CHUNK)]
        for n in range(net_count):
            mask = jnp.where(net == n, 1.0, 0.0).astype(BF16)
            X[n * paths : (n + 1) * paths, pl.ds(at, CHUNK)] = weighted * mask
        return carry

    lax.fori_loop(0, capacity // CHUNK, look_up, 0, unroll=2)

    def remote(src, dst, phase, tile, d, peer):
        return pltpu.make_async_remote_copy(
            src_ref=src,
            dst_ref=dst,
            send_sem=s_sems.at[phase, tile, d - 1],
            recv_sem=r_sems.at[phase, tile, d - 1],
            device_id={"trade": peer},
            device_id_type=MESH,
        )

    def mates(d):
        kx, ky = (x + d) % SIDE, (y + d) % SIDE
        return kx, ky, y * SIDE + kx, ky * SIDE + x

    def columns(t, width):
        at = t * TILE
        return pl.ds(at if isinstance(at, int) else pl.multiple_of(at, TILE), width)

    def stage1(t, width):
        cols = columns(t, width)
        for d in (2, 1, 3):
            kx, ky, in_row, in_column = mates(d)
            yield remote(S.at[:, kx, 0, :, cols], recv1.at[0, d - 1, :, :, cols], 0, t, d, in_row)
            yield remote(S.at[ky, :, 1, :, cols], recv1.at[1, d - 1, :, :, cols], 1, t, d, in_column)

    def stage2(t, width):
        cols = columns(t, width)
        for d in (2, 1, 3):
            kx, ky, in_row, in_column = mates(d)
            yield remote(st.at[0, ky, :, cols], recv2.at[0, d - 1, :, cols], 2, t, d, in_column)
            yield remote(st.at[1, kx, :, cols], recv2.at[1, d - 1, :, cols], 3, t, d, in_row)

    def gather1(t, width):
        cols = columns(t, width)
        own_a, own_b = G.at[y, x, 0, :, cols], G.at[y, x, 1, :, cols]
        for d in (2, 1, 3):
            kx, ky, in_row, in_column = mates(d)
            yield remote(own_a, own_a, 4, t, d, in_column)
            yield remote(own_b, own_b, 5, t, d, in_row)

    def gather2(t, width):
        cols = columns(t, width)
        all_a, all_b = G.at[:, x, 0, :, cols], G.at[y, :, 1, :, cols]
        for d in (2, 1, 3):
            kx, ky, in_row, in_column = mates(d)
            yield remote(all_a, all_a, 6, t, d, in_row)
            yield remote(all_b, all_b, 7, t, d, in_column)

    def start(copies):
        for copy in copies:
            copy.start()

    def arrive(copies):
        for copy in copies:
            copy.wait_recv()

    def pass_on(t, width):
        arrive(stage1(t, width))
        cols = columns(t, width)
        total_a = S[:, x, 0, :, cols].astype(F32)
        total_b = S[y, :, 1, :, cols].astype(F32)
        for d in range(OTHERS):
            total_a += recv1[0, d, :, :, cols].astype(F32)
            total_b += recv1[1, d, :, :, cols].astype(F32)
        st[0, :, :, cols] = total_a.astype(BF16)
        st[1, :, :, cols] = total_b.astype(BF16)
        start(stage2(t, width))

    last = len(tiles) - 1
    last_width = tiles[last][1]

    def forward(t, carry):
        at = pl.multiple_of(t * TILE, TILE)
        for i in range(capacity // CHUNK):
            part = pl.ds(i * CHUNK, CHUNK)
            bucket = wrow[:, part]
            sub = (at + lax.broadcasted_iota(jnp.int32, (TILE, CHUNK), 0)).astype(F32)
            hot[pl.ds(at, TILE), part] = jnp.where(sub == bucket, 1.0, 0.0).astype(BF16)
        result = dot(X[...], hot[pl.ds(at, TILE), :], NT)
        S[:, :, :, :, pl.ds(at, TILE)] = result.astype(BF16).reshape(S.shape[:-1] + (TILE,))

        @pl.when(t == 0)
        def _():
            pl.semaphore_wait(barrier, groups - 1 + slabs - 1)

        @pl.when(t < last)
        def _():
            start(stage1(t, TILE))

        @pl.when(t == last)
        def _():
            start(stage1(last, last_width))

        @pl.when(t > 0)
        def _():
            pass_on(t - 1, TILE)

        return carry

    lax.fori_loop(0, len(tiles), forward, 0)
    c_copy.wait()
    for at, width in tiles:
        block = C[:, at : at + width]
        high = block.astype(BF16)
        Chi[:, at : at + width] = high
        Clo[:, at : at + width] = (block - high.astype(F32)).astype(BF16)
    pass_on(last, last_width)
    for t, (at, width) in enumerate(tiles):
        arrive(stage2(t, width))
        cols = pl.ds(at, width)
        total_a = st[0, y, :, cols].astype(F32)
        total_b = st[1, x, :, cols].astype(F32)
        for d in range(OTHERS):
            total_a += recv2[0, d, :, cols].astype(F32)
            total_b += recv2[1, d, :, cols].astype(F32)
        SF[0 : own_rows // 2, cols] = total_a
        SF[own_rows // 2 : own_rows, cols] = total_b

    summed = SF[...]
    s_high = summed.astype(BF16)
    s_low = (summed - s_high.astype(F32)).astype(BF16)
    both = dot(jnp.concatenate([s_high, s_low], axis=0), Chi[...], NN)
    coupled = both[0:own_rows] + both[own_rows:] + dot(s_high, Clo[...], NN)
    margin = jnp.sqrt(jnp.sum(summed * coupled, axis=1, keepdims=True) + EPSILON)
    per_net = paths // own_rows
    own_net, own_part = me // per_net, me % per_net
    sub = lax.broadcasted_iota(jnp.int32, (own_rows, paths), 0)
    lane = lax.broadcasted_iota(jnp.int32, (own_rows, paths), 1)
    mine = lane == sub + own_part * own_rows
    net_sub = lax.broadcasted_iota(jnp.int32, (net_count, paths), 0)
    cot_row = jnp.sum(jnp.where(net_sub == own_net, cot[...], 0.0), axis=0, keepdims=True)
    cot_column = jnp.sum(jnp.where(mine, cot_row, 0.0), axis=1, keepdims=True)
    grad = ((cot_column / margin) * coupled).astype(BF16)
    G[y, x, :, :, 0:bucket_count] = grad.reshape(2, own_rows // 2, bucket_count)

    for t, (at, width) in enumerate(tiles):
        start(gather1(t, width))

    margin_row = jnp.sum(jnp.where(mine, margin, 0.0), axis=0, keepdims=True)
    my_margins = jnp.where(net_sub == own_net, margin_row, 0.0)
    m_send[...] = my_margins
    m_copies = []
    for d in range(1, groups):
        copy = pltpu.make_async_remote_copy(
            src_ref=m_send,
            dst_ref=m_recv.at[d - 1],
            send_sem=ms_sems.at[d - 1],
            recv_sem=mr_sems.at[d - 1],
            device_id={"trade": (me + d) % groups},
            device_id_type=MESH,
        )
        copy.start()
        m_copies.append(copy)

    for t, (at, width) in enumerate(tiles):
        arrive(gather1(t, width))
        start(gather2(t, width))
    e_copies = []
    for copy in m_copies:
        copy.wait_recv()
    all_margins = my_margins
    for d in range(groups - 1):
        all_margins += m_recv[d]
    margin_o[...] = all_margins
    my_sum = jnp.sum(all_margins * pw[...], axis=1, keepdims=True)
    e_send[...] = jnp.broadcast_to(my_sum, e_send.shape)
    for d in range(1, slabs):
        copy = pltpu.make_async_remote_copy(
            src_ref=e_send,
            dst_ref=e_recv.at[d - 1],
            send_sem=es_sems.at[d - 1],
            recv_sem=er_sems.at[d - 1],
            device_id={"path": (slab + d) % slabs},
            device_id_type=MESH,
        )
        copy.start()
        e_copies.append(copy)

    def backward(t, carry):
        @pl.when(t < last)
        def _():
            arrive(gather2(t, TILE))

        @pl.when(t == last)
        def _():
            arrive(gather2(last, last_width))

        at = pl.multiple_of(t * TILE, TILE)

        def one(i, carry):
            part = pl.ds(pl.multiple_of(i * CHUNK, CHUNK), CHUNK)
            all_grad = G[:, :, :, :, pl.ds(at, TILE)].reshape(rows, TILE)
            looked_up = dot(all_grad, hot[pl.ds(at, TILE), part], NN)
            net = nets[:, part]
            total = acc[:, part]
            for n in range(net_count):
                total += jnp.where(net == n, looked_up[n * paths : (n + 1) * paths], 0.0)
            acc[:, part] = total
            return carry

        return lax.fori_loop(0, capacity // CHUNK, one, carry, unroll=2)

    lax.fori_loop(0, len(tiles), backward, 0)
    chosen_o[...] = acc[...].astype(BF16)

    for copy in e_copies:
        copy.wait_recv()
    everyone = e_send[...]
    for d in range(slabs - 1):
        everyone += e_recv[d]
    expected_o[...] = everyone / (paths * slabs)

    for t, (at, width) in enumerate(tiles):
        for stage in (stage1, stage2, gather1, gather2):
            for copy in stage(t, width):
                copy.wait_send()
    for copy in m_copies + e_copies:
        copy.wait_send()


def finish(weight, chosen, margin, expected, grad_o, margin_o, expected_o):
    scaled = chosen[...].astype(F32) * weight[...]
    grad_o[...] = scaled.T.astype(BF16)
    margin_o[...] = margin[...]
    net_count = margin.shape[0]
    sub = lax.broadcasted_iota(jnp.int32, margin.shape, 0)
    lane = lax.broadcasted_iota(jnp.int32, margin.shape, 1)
    row = jnp.sum(jnp.where(sub == lane, expected[...], 0.0), axis=0, keepdims=True)
    expected_o[...] = row[:, 0:net_count]


def shards(groups, slabs, deltas, net_ids, block_ids, bucket_map, risk_weight, counts, correlation, path_weight, margin_cotangent):
    capacity, paths = deltas.shape
    buckets = correlation.shape[0]
    net_count = margin_cotangent.shape[0]
    rows = net_count * paths
    half = rows // groups // 2
    tile_count = len(tiles_of(buckets))
    padded = tile_count * TILE
    vmem = pl.BlockSpec(memory_space=pltpu.VMEM)
    smem = pl.BlockSpec(memory_space=pltpu.SMEM)
    dma = pltpu.SemaphoreType.DMA
    anywhere = pl.BlockSpec(memory_space=pl.ANY)
    margin, expected, weight, chosen = pl.pallas_call(
        functools.partial(kernel, groups, slabs),
        out_shape=(
            jax.ShapeDtypeStruct((net_count, paths), F32),
            jax.ShapeDtypeStruct((net_count, paths), F32),
            jax.ShapeDtypeStruct((1, capacity), F32),
            jax.ShapeDtypeStruct((paths, capacity), BF16),
        ),
        in_specs=[anywhere, vmem, vmem, vmem, vmem, smem, anywhere, vmem, vmem],
        out_specs=(vmem, vmem, vmem, vmem),
        scratch_shapes=[
            pltpu.VMEM((capacity, paths), BF16),
            pltpu.VMEM((4 * LANES, LANES), BF16),
            pltpu.VMEM((padded, capacity), BF16),
            pltpu.VMEM((rows, capacity), BF16),
            pltpu.VMEM((1, capacity), F32),
            pltpu.VMEM((SIDE, SIDE, 2, half, padded), BF16),
            pltpu.VMEM((2, OTHERS, SIDE, half, buckets), BF16),
            pltpu.VMEM((2, SIDE, half, buckets), BF16),
            pltpu.VMEM((2, OTHERS, half, buckets), BF16),
            pltpu.VMEM((2 * half, buckets), F32),
            pltpu.VMEM((buckets, buckets), F32),
            pltpu.VMEM((buckets, buckets), BF16),
            pltpu.VMEM((buckets, buckets), BF16),
            pltpu.VMEM((SIDE, SIDE, 2, half, padded), BF16),
            pltpu.VMEM((paths, capacity), F32),
            pltpu.VMEM((net_count, paths), F32),
            pltpu.VMEM((groups - 1, net_count, paths), F32),
            pltpu.VMEM((net_count, paths), F32),
            pltpu.VMEM((slabs - 1, net_count, paths), F32),
            dma,
            dma,
            dma((8, tile_count, OTHERS)),
            dma((8, tile_count, OTHERS)),
            dma((groups - 1,)),
            dma((groups - 1,)),
            dma((slabs - 1,)),
            dma((slabs - 1,)),
        ],
        compiler_params=pltpu.CompilerParams(
            collective_id=0, has_side_effects=True, vmem_limit_bytes=60 * 1024 * 1024
        ),
        name="margin_exchange",
    )(
        deltas,
        net_ids.reshape(1, capacity),
        block_ids.reshape(1, capacity),
        risk_weight.reshape(-1, LANES),
        bucket_map.reshape(-1, LANES),
        counts,
        correlation,
        path_weight.reshape(1, paths),
        margin_cotangent,
    )
    block = capacity // 4
    whole = pl.BlockSpec((net_count, paths), lambda i: (0, 0))
    trade_grad, margin, expected = pl.pallas_call(
        finish,
        grid=(capacity // block,),
        out_shape=(
            jax.ShapeDtypeStruct((capacity, paths), BF16),
            jax.ShapeDtypeStruct((net_count, paths), F32),
            jax.ShapeDtypeStruct((1, net_count), F32),
        ),
        in_specs=[
            pl.BlockSpec((1, block), lambda i: (0, i)),
            pl.BlockSpec((paths, block), lambda i: (0, i)),
            whole,
            whole,
        ],
        out_specs=(
            pl.BlockSpec((block, paths), lambda i: (i, 0)),
            whole,
            pl.BlockSpec((1, net_count), lambda i: (0, 0)),
        ),
        name="finish",
    )(weight, chosen, margin, expected)
    return margin, expected.reshape(net_count), trade_grad


def solution(mesh):
    placed = (
        P("trade", "path"),
        P("trade"),
        P("trade"),
        P(),
        P(),
        P("trade"),
        P(),
        P("path"),
        P(None, "path"),
    )
    return jax.shard_map(
        functools.partial(shards, mesh.shape["trade"], mesh.shape["path"]),
        mesh=mesh,
        in_specs=placed,
        out_specs=(P(None, "path"), P(), P("trade", "path")),
        check_vma=False,
    )
```

```python
import functools

import jax
import jax.numpy as jnp
from jax import lax
from jax.experimental import pallas as pl
from jax.experimental.pallas import tpu as pltpu
from jax.sharding import PartitionSpec as P

EPSILON = 1e-06
LANES = 128
F32 = jnp.float32
BF16 = jnp.bfloat16
MESH = pl.DeviceIdType.MESH
SIDE = 4
OTHERS = SIDE - 1
CHUNK = 512
NT = (((1,), (1,)), ((), ()))
NN = (((1,), (0,)), ((), ()))
TN = (((0,), (0,)), ((), ()))


def dot(a, b, dims):
    return lax.dot_general(a, b, dims, preferred_element_type=F32)


TILE = 256
LAG = 3
STEP = 1024


def tiles_of(total):
    cuts, at = [], 0
    while at < total:
        width = min(TILE, total - at)
        cuts.append((at, width))
        at += width
    return cuts


def kernel(
    groups,
    slabs,
    deltas_in,
    nets_in,
    blocks_in,
    rw_in,
    bm_in,
    counts,
    corr,
    pw_in,
    cot_in,
    margin_o,
    expected_o,
    grad_o,
    slots,
    nets,
    blocks,
    rw,
    bm,
    pw,
    cot,
    weight,
    table,
    hot,
    X,
    wrow,
    S,
    recv1,
    st,
    recv2,
    SF,
    C,
    Chi,
    Clo,
    G,
    acc,
    m_send,
    m_recv,
    e_send,
    e_recv,
    c_sem,
    in_sems,
    s_sems,
    r_sems,
    ms_sems,
    mr_sems,
    es_sems,
    er_sems,
):
    me = lax.axis_index("trade")
    slab = lax.axis_index("path")
    y, x = me // SIDE, me % SIDE
    capacity = slots.shape[0]
    bucket_count = corr.shape[0]
    net_count, paths = cot.shape
    rows = net_count * paths
    own_rows = rows // groups
    tiles = tiles_of(bucket_count)

    entering = [
        pltpu.make_async_copy(source, target, in_sems.at[i])
        for i, (source, target) in enumerate(
            (
                (rw_in, rw),
                (bm_in, bm),
                (blocks_in, blocks),
                (nets_in, nets),
                (deltas_in, slots),
                (pw_in, pw),
                (cot_in, cot),
            )
        )
    ]
    for copy in entering:
        copy.start()
    c_copy = pltpu.make_async_copy(corr, C, c_sem)
    c_copy.start()

    barrier = pltpu.get_barrier_semaphore()
    for d in range(1, groups):
        pl.semaphore_signal(barrier, inc=1, device_id={"trade": (me + d) % groups}, device_id_type=MESH)
    for d in range(1, slabs):
        pl.semaphore_signal(barrier, inc=1, device_id={"path": (slab + d) % slabs}, device_id_type=MESH)

    acc[...] = jnp.zeros_like(acc)
    table[...] = jnp.zeros_like(table)
    padded = hot.shape[0]
    if padded > bucket_count:
        G[:, :, :, :, bucket_count:padded] = jnp.zeros(G.shape[:-1] + (padded - bucket_count,), BF16)
    for copy in entering:
        copy.wait()
    table_rows = rw.shape[0]
    w_all = rw[...]
    w1 = w_all.astype(BF16).astype(F32)
    b_all = bm[...]
    parts = (w1, w_all - w1, (b_all // LANES).astype(F32), (b_all % LANES).astype(F32))
    for k, part in enumerate(parts):
        table[k * LANES : (k + 1) * LANES, 0:table_rows] = part.T.astype(BF16)
    live_count = counts[0]

    def look_up(i, carry):
        at = pl.multiple_of(i * CHUNK, CHUNK)
        ids = blocks[:, pl.ds(at, CHUNK)]
        high, low = ids // LANES, ids % LANES
        sub = lax.broadcasted_iota(jnp.int32, (LANES, CHUNK), 0)
        pick = jnp.where(sub == high, 1.0, 0.0).astype(BF16)
        found = dot(table[...], pick, NN)
        keep = sub == low
        parts = [
            jnp.sum(jnp.where(keep, found[k * LANES : (k + 1) * LANES], 0.0), axis=0, keepdims=True)
            for k in range(4)
        ]
        slot = at + lax.broadcasted_iota(jnp.int32, (1, CHUNK), 1)
        w = jnp.where(slot < live_count, parts[0] + parts[1], 0.0)
        weight[:, pl.ds(at, CHUNK)] = w
        wrow[:, pl.ds(at, CHUNK)] = parts[2] * LANES + parts[3]
        turned = slots[pl.ds(at, CHUNK), :].T.astype(F32)
        weighted = (turned * w).astype(BF16)
        net = nets[:, pl.ds(at, CHUNK)]
        for n in range(net_count):
            mask = jnp.where(net == n, 1.0, 0.0).astype(BF16)
            X[n * paths : (n + 1) * paths, pl.ds(at, CHUNK)] = weighted * mask
        return carry

    lax.fori_loop(0, capacity // CHUNK, look_up, 0, unroll=4)

    def remote(src, dst, phase, tile, d, peer):
        return pltpu.make_async_remote_copy(
            src_ref=src,
            dst_ref=dst,
            send_sem=s_sems.at[phase, tile, d - 1],
            recv_sem=r_sems.at[phase, tile, d - 1],
            device_id={"trade": peer},
            device_id_type=MESH,
        )

    def mates(d):
        kx, ky = (x + d) % SIDE, (y + d) % SIDE
        return kx, ky, y * SIDE + kx, ky * SIDE + x

    def columns(t, width):
        at = t * TILE
        return pl.ds(at if isinstance(at, int) else pl.multiple_of(at, TILE), width)

    def stage1(t, width):
        cols = columns(t, width)
        for d in (2, 1, 3):
            kx, ky, in_row, in_column = mates(d)
            yield remote(S.at[:, kx, 0, :, cols], recv1.at[0, d - 1, :, :, cols], 0, t, d, in_row)
            yield remote(S.at[ky, :, 1, :, cols], recv1.at[1, d - 1, :, :, cols], 1, t, d, in_column)

    def stage2(t, width):
        cols = columns(t, width)
        for d in (2, 1, 3):
            kx, ky, in_row, in_column = mates(d)
            yield remote(st.at[0, ky, :, cols], recv2.at[0, d - 1, :, cols], 2, t, d, in_column)
            yield remote(st.at[1, kx, :, cols], recv2.at[1, d - 1, :, cols], 3, t, d, in_row)

    def gather1(t, width):
        cols = columns(t, width)
        own_a, own_b = G.at[y, x, 0, :, cols], G.at[y, x, 1, :, cols]
        for d in (2, 1, 3):
            kx, ky, in_row, in_column = mates(d)
            yield remote(own_a, own_a, 4, t, d, in_column)
            yield remote(own_b, own_b, 5, t, d, in_row)

    def gather2(t, width):
        cols = columns(t, width)
        all_a, all_b = G.at[:, x, 0, :, cols], G.at[y, :, 1, :, cols]
        for d in (2, 1, 3):
            kx, ky, in_row, in_column = mates(d)
            yield remote(all_a, all_a, 6, t, d, in_row)
            yield remote(all_b, all_b, 7, t, d, in_column)

    def start(copies):
        for copy in copies:
            copy.start()

    def arrive(copies):
        for copy in copies:
            copy.wait_recv()

    def pass_on(t, width):
        arrive(stage1(t, width))
        cols = columns(t, width)
        total_a = S[:, x, 0, :, cols].astype(F32)
        total_b = S[y, :, 1, :, cols].astype(F32)
        for d in range(OTHERS):
            total_a += recv1[0, d, :, :, cols].astype(F32)
            total_b += recv1[1, d, :, :, cols].astype(F32)
        st[0, :, :, cols] = total_a.astype(BF16)
        st[1, :, :, cols] = total_b.astype(BF16)
        start(stage2(t, width))

    last = len(tiles) - 1
    last_width = tiles[last][1]

    def forward(t, carry):
        at = pl.multiple_of(t * TILE, TILE)
        for i in range(capacity // CHUNK):
            part = pl.ds(i * CHUNK, CHUNK)
            bucket = wrow[:, part]
            sub = (at + lax.broadcasted_iota(jnp.int32, (TILE, CHUNK), 0)).astype(F32)
            hot[pl.ds(at, TILE), part] = jnp.where(sub == bucket, 1.0, 0.0).astype(BF16)
        result = dot(X[...], hot[pl.ds(at, TILE), :], NT)
        S[:, :, :, :, pl.ds(at, TILE)] = result.astype(BF16).reshape(S.shape[:-1] + (TILE,))

        @pl.when(t == 0)
        def _():
            pl.semaphore_wait(barrier, groups - 1 + slabs - 1)

        @pl.when(t < last)
        def _():
            start(stage1(t, TILE))

        @pl.when(t == last)
        def _():
            start(stage1(last, last_width))

        @pl.when(t >= LAG)
        def _():
            pass_on(t - LAG, TILE)

        return carry

    lax.fori_loop(0, len(tiles), forward, 0)
    c_copy.wait()
    for at, width in tiles:
        block = C[:, at : at + width]
        high = block.astype(BF16)
        Chi[:, at : at + width] = high
        Clo[:, at : at + width] = (block - high.astype(F32)).astype(BF16)
    for t in range(len(tiles) - LAG, len(tiles)):
        pass_on(t, tiles[t][1])
    for t, (at, width) in enumerate(tiles):
        arrive(stage2(t, width))
        cols = pl.ds(at, width)
        total_a = st[0, y, :, cols].astype(F32)
        total_b = st[1, x, :, cols].astype(F32)
        for d in range(OTHERS):
            total_a += recv2[0, d, :, cols].astype(F32)
            total_b += recv2[1, d, :, cols].astype(F32)
        SF[0 : own_rows // 2, cols] = total_a
        SF[own_rows // 2 : own_rows, cols] = total_b

    summed = SF[...]
    s_high = summed.astype(BF16)
    s_low = (summed - s_high.astype(F32)).astype(BF16)
    both = dot(jnp.concatenate([s_high, s_low], axis=0), Chi[...], NN)
    coupled = both[0:own_rows] + both[own_rows:] + dot(s_high, Clo[...], NN)
    margin = jnp.sqrt(jnp.sum(summed * coupled, axis=1, keepdims=True) + EPSILON)
    per_net = paths // own_rows
    own_net, own_part = me // per_net, me % per_net
    sub = lax.broadcasted_iota(jnp.int32, (own_rows, paths), 0)
    lane = lax.broadcasted_iota(jnp.int32, (own_rows, paths), 1)
    mine = lane == sub + own_part * own_rows
    net_sub = lax.broadcasted_iota(jnp.int32, (net_count, paths), 0)
    cot_row = jnp.sum(jnp.where(net_sub == own_net, cot[...], 0.0), axis=0, keepdims=True)
    cot_column = jnp.sum(jnp.where(mine, cot_row, 0.0), axis=1, keepdims=True)
    grad = ((cot_column / margin) * coupled).astype(BF16)
    G[y, x, :, :, 0:bucket_count] = grad.reshape(2, own_rows // 2, bucket_count)

    for t in reversed(range(len(tiles))):
        start(gather1(t, tiles[t][1]))

    margin_row = jnp.sum(jnp.where(mine, margin, 0.0), axis=0, keepdims=True)
    my_margins = jnp.where(net_sub == own_net, margin_row, 0.0)
    m_send[...] = my_margins

    def margin_copies():
        for d in range(1, groups):
            yield pltpu.make_async_remote_copy(
                src_ref=m_send,
                dst_ref=m_recv.at[d - 1],
                send_sem=ms_sems.at[d - 1],
                recv_sem=mr_sems.at[d - 1],
                device_id={"trade": (me + d) % groups},
                device_id_type=MESH,
            )

    for t in reversed(range(len(tiles))):
        arrive(gather1(t, tiles[t][1]))
        start(gather2(t, tiles[t][1]))
        if t == last:
            start(margin_copies())
    def mean_copies():
        for d in range(1, slabs):
            yield pltpu.make_async_remote_copy(
                src_ref=e_send,
                dst_ref=e_recv.at[d - 1],
                send_sem=es_sems.at[d - 1],
                recv_sem=er_sems.at[d - 1],
                device_id={"path": (slab + d) % slabs},
                device_id_type=MESH,
            )

    def margins():
        arrive(margin_copies())
        all_margins = m_send[...]
        for d in range(groups - 1):
            all_margins += m_recv[d]
        margin_o[...] = all_margins
        my_sum = jnp.sum(all_margins * pw[...], axis=1, keepdims=True)
        e_send[...] = jnp.broadcast_to(my_sum, e_send.shape)
        start(mean_copies())

    def backward(i, carry):
        t = last - i

        @pl.when(t < last)
        def _():
            arrive(gather2(t, TILE))

        @pl.when(t == last)
        def _():
            arrive(gather2(last, last_width))

        at = pl.multiple_of(t * TILE, TILE)

        def one(i, carry):
            part = pl.ds(pl.multiple_of(i * STEP, STEP), STEP)
            all_grad = G[:, :, :, :, pl.ds(at, TILE)].reshape(rows, TILE)
            looked_up = dot(all_grad, hot[pl.ds(at, TILE), part], NN)
            net = nets[:, part]
            total = acc[:, part]
            for n in range(net_count):
                total += jnp.where(net == n, looked_up[n * paths : (n + 1) * paths], 0.0)
            acc[:, part] = total
            return carry

        lax.fori_loop(0, capacity // STEP, one, carry, unroll=2)

        @pl.when(i == 1)
        def _():
            margins()

        return carry

    lax.fori_loop(0, len(tiles), backward, 0)
    grad_o[...] = (acc[...] * weight[...]).astype(BF16)

    arrive(mean_copies())
    everyone = e_send[...]
    for d in range(slabs - 1):
        everyone += e_recv[d]
    expected_o[...] = everyone / (paths * slabs)

    for t, (at, width) in enumerate(tiles):
        for stage in (stage1, stage2, gather1, gather2):
            for copy in stage(t, width):
                copy.wait_send()
    for copy in (*margin_copies(), *mean_copies()):
        copy.wait_send()


def finish(grad, margin, expected, grad_o, margin_o, expected_o):
    block = grad_o.shape[0]
    at = pl.multiple_of(pl.program_id(0) * block, block)
    grad_o[...] = grad[:, pl.ds(at, block)].T
    margin_o[...] = margin[...]
    net_count = margin.shape[0]
    sub = lax.broadcasted_iota(jnp.int32, margin.shape, 0)
    lane = lax.broadcasted_iota(jnp.int32, margin.shape, 1)
    row = jnp.sum(jnp.where(sub == lane, expected[...], 0.0), axis=0, keepdims=True)
    expected_o[...] = row[:, 0:net_count]


def shards(groups, slabs, deltas, net_ids, block_ids, bucket_map, risk_weight, counts, correlation, path_weight, margin_cotangent):
    capacity, paths = deltas.shape
    buckets = correlation.shape[0]
    net_count = margin_cotangent.shape[0]
    rows = net_count * paths
    half = rows // groups // 2
    tile_count = len(tiles_of(buckets))
    padded = tile_count * TILE
    vmem = pl.BlockSpec(memory_space=pltpu.VMEM)
    smem = pl.BlockSpec(memory_space=pltpu.SMEM)
    dma = pltpu.SemaphoreType.DMA
    anywhere = pl.BlockSpec(memory_space=pl.ANY)
    margin, expected, turned_grad = pl.pallas_call(
        functools.partial(kernel, groups, slabs),
        out_shape=(
            jax.ShapeDtypeStruct((net_count, paths), F32),
            jax.ShapeDtypeStruct((net_count, paths), F32),
            jax.ShapeDtypeStruct((paths, capacity), BF16),
        ),
        in_specs=[anywhere] * 5 + [smem] + [anywhere] * 3,
        out_specs=(vmem, vmem, vmem),
        scratch_shapes=[
            pltpu.VMEM((capacity, paths), BF16),
            pltpu.VMEM((1, capacity), jnp.int32),
            pltpu.VMEM((1, capacity), jnp.int32),
            pltpu.VMEM((risk_weight.size // LANES, LANES), F32),
            pltpu.VMEM((bucket_map.size // LANES, LANES), jnp.int32),
            pltpu.VMEM((1, paths), F32),
            pltpu.VMEM((net_count, paths), F32),
            pltpu.VMEM((1, capacity), F32),
            pltpu.VMEM((4 * LANES, LANES), BF16),
            pltpu.VMEM((padded, capacity), BF16),
            pltpu.VMEM((rows, capacity), BF16),
            pltpu.VMEM((1, capacity), F32),
            pltpu.VMEM((SIDE, SIDE, 2, half, padded), BF16),
            pltpu.VMEM((2, OTHERS, SIDE, half, buckets), BF16),
            pltpu.VMEM((2, SIDE, half, buckets), BF16),
            pltpu.VMEM((2, OTHERS, half, buckets), BF16),
            pltpu.VMEM((2 * half, buckets), F32),
            pltpu.VMEM((buckets, buckets), F32),
            pltpu.VMEM((buckets, buckets), BF16),
            pltpu.VMEM((buckets, buckets), BF16),
            pltpu.VMEM((SIDE, SIDE, 2, half, padded), BF16),
            pltpu.VMEM((paths, capacity), F32),
            pltpu.VMEM((net_count, paths), F32),
            pltpu.VMEM((groups - 1, net_count, paths), F32),
            pltpu.VMEM((net_count, paths), F32),
            pltpu.VMEM((slabs - 1, net_count, paths), F32),
            dma,
            dma((7,)),
            dma((8, tile_count, OTHERS)),
            dma((8, tile_count, OTHERS)),
            dma((groups - 1,)),
            dma((groups - 1,)),
            dma((slabs - 1,)),
            dma((slabs - 1,)),
        ],
        compiler_params=pltpu.CompilerParams(
            collective_id=0, has_side_effects=True, vmem_limit_bytes=52 * 1024 * 1024
        ),
        name="margin_exchange",
    )(
        deltas,
        net_ids.reshape(1, capacity),
        block_ids.reshape(1, capacity),
        risk_weight.reshape(-1, LANES),
        bucket_map.reshape(-1, LANES),
        counts,
        correlation,
        path_weight.reshape(1, paths),
        margin_cotangent,
    )
    block = capacity // 2
    whole = pl.BlockSpec((net_count, paths), lambda i: (0, 0))
    trade_grad, margin, expected = pl.pallas_call(
        finish,
        grid=(capacity // block,),
        out_shape=(
            jax.ShapeDtypeStruct((capacity, paths), BF16),
            jax.ShapeDtypeStruct((net_count, paths), F32),
            jax.ShapeDtypeStruct((1, net_count), F32),
        ),
        in_specs=[vmem, vmem, vmem],
        out_specs=(
            pl.BlockSpec((block, paths), lambda i: (i, 0)),
            whole,
            pl.BlockSpec((1, net_count), lambda i: (0, 0)),
        ),
        compiler_params=pltpu.CompilerParams(vmem_limit_bytes=8 * 1024 * 1024),
        name="finish",
    )(turned_grad, margin, expected)
    return margin, expected.reshape(net_count), trade_grad


def solution(mesh):
    placed = (
        P("trade", "path"),
        P("trade"),
        P("trade"),
        P(),
        P(),
        P("trade"),
        P(),
        P("path"),
        P(None, "path"),
    )
    return jax.shard_map(
        functools.partial(shards, mesh.shape["trade"], mesh.shape["path"]),
        mesh=mesh,
        in_specs=placed,
        out_specs=(P(None, "path"), P(), P("trade", "path")),
        check_vma=False,
    )
```

```python
import functools

import jax
import jax.numpy as jnp
from jax import lax
from jax.experimental import pallas as pl
from jax.experimental.pallas import tpu as pltpu
from jax.sharding import PartitionSpec as P

EPSILON = 1e-06
LANES = 128
F32 = jnp.float32
BF16 = jnp.bfloat16
MESH = pl.DeviceIdType.MESH
SIDE = 4
OTHERS = SIDE - 1
CHUNK = 512
NT = (((1,), (1,)), ((), ()))
NN = (((1,), (0,)), ((), ()))
TN = (((0,), (0,)), ((), ()))


def dot(a, b, dims):
    return lax.dot_general(a, b, dims, preferred_element_type=F32)


TILE = 256
HALVES = 2
LAG = 3
STEP = 2048
AHEAD = 2
SPREAD_AT = 3
MARGINS_AT = 6


def tiles_of(total):
    cuts, at = [], 0
    while at < total:
        width = min(TILE, total - at)
        cuts.append((at, width))
        at += width
    return cuts


def kernel(
    groups,
    slabs,
    deltas_in,
    nets_in,
    blocks_in,
    rw_in,
    bm_in,
    counts,
    corr,
    pw_in,
    cot_in,
    margin_o,
    expected_o,
    grad_o,
    slots,
    nets,
    blocks,
    rw,
    bm,
    pw,
    cot,
    weight,
    table,
    hot,
    X,
    wrow,
    S,
    recv1,
    st,
    recv2,
    SF,
    C,
    Chi,
    Clo,
    G,
    acc,
    m_send,
    m_recv,
    e_send,
    e_recv,
    c_sem,
    in_sems,
    s_sems,
    r_sems,
    ms_sems,
    mr_sems,
    es_sems,
    er_sems,
):
    me = lax.axis_index("trade")
    slab = lax.axis_index("path")
    y, x = me // SIDE, me % SIDE
    capacity = slots.shape[0]
    bucket_count = corr.shape[0]
    net_count, paths = cot.shape
    rows = net_count * paths
    half_rows = rows // HALVES
    half_nets = net_count // HALVES
    own_rows = half_rows // groups
    quarter = own_rows // 2
    tiles = tiles_of(bucket_count)

    entering = [
        pltpu.make_async_copy(source, target, in_sems.at[i])
        for i, (source, target) in enumerate(
            (
                (rw_in, rw),
                (bm_in, bm),
                (blocks_in, blocks),
                (nets_in, nets),
                (deltas_in, slots),
                (pw_in, pw),
                (cot_in, cot),
            )
        )
    ]
    for copy in entering:
        copy.start()
    c_copy = pltpu.make_async_copy(corr, C, c_sem)
    c_copy.start()

    barrier = pltpu.get_barrier_semaphore()
    for d in range(1, groups):
        pl.semaphore_signal(barrier, inc=1, device_id={"trade": (me + d) % groups}, device_id_type=MESH)
    for d in range(1, slabs):
        pl.semaphore_signal(barrier, inc=1, device_id={"path": (slab + d) % slabs}, device_id_type=MESH)

    acc[...] = jnp.zeros_like(acc)
    table[...] = jnp.zeros_like(table)
    padded = hot.shape[0]
    if padded > bucket_count:
        G[:, :, :, :, :, bucket_count:padded] = jnp.zeros(G.shape[:-1] + (padded - bucket_count,), BF16)
    for copy in entering:
        copy.wait()
    table_rows = rw.shape[0]
    w_all = rw[...]
    w1 = w_all.astype(BF16).astype(F32)
    b_all = bm[...]
    parts = (w1, w_all - w1, (b_all // LANES).astype(F32), (b_all % LANES).astype(F32))
    for k, part in enumerate(parts):
        table[k * LANES : (k + 1) * LANES, 0:table_rows] = part.T.astype(BF16)
    live_count = counts[0]

    def look_up(i, carry):
        at = pl.multiple_of(i * CHUNK, CHUNK)
        ids = blocks[:, pl.ds(at, CHUNK)]
        high, low = ids // LANES, ids % LANES
        sub = lax.broadcasted_iota(jnp.int32, (LANES, CHUNK), 0)
        pick = jnp.where(sub == high, 1.0, 0.0).astype(BF16)
        found = dot(table[...], pick, NN)
        keep = sub == low
        parts = [
            jnp.sum(jnp.where(keep, found[k * LANES : (k + 1) * LANES], 0.0), axis=0, keepdims=True)
            for k in range(4)
        ]
        slot = at + lax.broadcasted_iota(jnp.int32, (1, CHUNK), 1)
        w = jnp.where(slot < live_count, parts[0] + parts[1], 0.0)
        weight[:, pl.ds(at, CHUNK)] = w
        wrow[:, pl.ds(at, CHUNK)] = parts[2] * LANES + parts[3]
        turned = slots[pl.ds(at, CHUNK), :].T.astype(F32)
        weighted = (turned * w).astype(BF16)
        net = nets[:, pl.ds(at, CHUNK)]
        for n in range(net_count):
            mask = jnp.where(net == n, 1.0, 0.0).astype(BF16)
            X[n * paths : (n + 1) * paths, pl.ds(at, CHUNK)] = weighted * mask
        return carry

    lax.fori_loop(0, capacity // CHUNK, look_up, 0, unroll=4)

    def remote(src, dst, phase, tile, d, peer):
        return pltpu.make_async_remote_copy(
            src_ref=src,
            dst_ref=dst,
            send_sem=s_sems.at[phase, tile, d - 1],
            recv_sem=r_sems.at[phase, tile, d - 1],
            device_id={"trade": peer},
            device_id_type=MESH,
        )

    def mates(d):
        kx, ky = (x + d) % SIDE, (y + d) % SIDE
        return kx, ky, y * SIDE + kx, ky * SIDE + x

    def columns(t, width):
        at = t * TILE
        return pl.ds(at if isinstance(at, int) else pl.multiple_of(at, TILE), width)

    steps = len(tiles)
    last = steps - 1
    last_width = tiles[last][1]

    def stage1(h, t, width):
        cols, i = columns(t, width), h * steps + t
        for d in (2, 1, 3):
            kx, ky, in_row, in_column = mates(d)
            yield remote(S.at[h, :, kx, 0, :, cols], recv1.at[h, 0, d - 1, :, :, cols], 0, i, d, in_row)
            yield remote(S.at[h, ky, :, 1, :, cols], recv1.at[h, 1, d - 1, :, :, cols], 1, i, d, in_column)

    def stage2(h, t, width):
        cols, i = columns(t, width), h * steps + t
        for d in (2, 1, 3):
            kx, ky, in_row, in_column = mates(d)
            yield remote(st.at[h, 0, ky, :, cols], recv2.at[h, 0, d - 1, :, cols], 2, i, d, in_column)
            yield remote(st.at[h, 1, kx, :, cols], recv2.at[h, 1, d - 1, :, cols], 3, i, d, in_row)

    def gather1(h, t, width):
        cols, i = columns(t, width), h * steps + t
        own_a, own_b = G.at[h, y, x, 0, :, cols], G.at[h, y, x, 1, :, cols]
        for d in (2, 1, 3):
            kx, ky, in_row, in_column = mates(d)
            yield remote(own_a, own_a, 4, i, d, in_column)
            yield remote(own_b, own_b, 5, i, d, in_row)

    def gather2(h, t, width):
        cols, i = columns(t, width), h * steps + t
        all_a, all_b = G.at[h, :, x, 0, :, cols], G.at[h, y, :, 1, :, cols]
        for d in (2, 1, 3):
            kx, ky, in_row, in_column = mates(d)
            yield remote(all_a, all_a, 6, i, d, in_row)
            yield remote(all_b, all_b, 7, i, d, in_column)

    def start(copies):
        for copy in copies:
            copy.start()

    def arrive(copies):
        for copy in copies:
            copy.wait_recv()

    def by_width(i, run):
        h, t = i // steps, i % steps

        @pl.when(t < last)
        def _():
            run(h, t, TILE)

        @pl.when(t == last)
        def _():
            run(h, last, last_width)

    def pass_on(h, t, width):
        arrive(stage1(h, t, width))
        cols = columns(t, width)
        total_a = S[h, :, x, 0, :, cols].astype(F32)
        total_b = S[h, y, :, 1, :, cols].astype(F32)
        for d in range(OTHERS):
            total_a += recv1[h, 0, d, :, :, cols].astype(F32)
            total_b += recv1[h, 1, d, :, :, cols].astype(F32)
        st[h, 0, :, :, cols] = total_a.astype(BF16)
        st[h, 1, :, :, cols] = total_b.astype(BF16)
        start(stage2(h, t, width))

    def forward(i, carry):
        h, t = i // steps, i % steps
        at = pl.multiple_of(t * TILE, TILE)

        @pl.when(h == 0)
        def _():
            for k in range(capacity // CHUNK):
                part = pl.ds(k * CHUNK, CHUNK)
                bucket = wrow[:, part]
                sub = (at + lax.broadcasted_iota(jnp.int32, (TILE, CHUNK), 0)).astype(F32)
                hot[pl.ds(at, TILE), part] = jnp.where(sub == bucket, 1.0, 0.0).astype(BF16)

        half = pl.ds(pl.multiple_of(h * half_rows, half_rows), half_rows)
        result = dot(X[half, :], hot[pl.ds(at, TILE), :], NT).astype(BF16)
        S[h, :, :, :, :, pl.ds(at, TILE)] = result.reshape(S.shape[1:-1] + (TILE,))

        @pl.when(i == 0)
        def _():
            pl.semaphore_wait(barrier, groups - 1 + slabs - 1)

        by_width(i, lambda h, t, width: start(stage1(h, t, width)))

        @pl.when(i >= LAG)
        def _():
            by_width(i - LAG, pass_on)

        return carry

    total_steps = HALVES * steps
    lax.fori_loop(0, total_steps, forward, 0)
    c_copy.wait()
    for at, width in tiles:
        block = C[:, at : at + width]
        high = block.astype(BF16)
        Chi[:, at : at + width] = high
        Clo[:, at : at + width] = (block - high.astype(F32)).astype(BF16)

    per_net = paths // own_rows
    own_part = me % per_net
    sub = lax.broadcasted_iota(jnp.int32, (own_rows, paths), 0)
    lane = lax.broadcasted_iota(jnp.int32, (own_rows, paths), 1)
    mine = lane == sub + own_part * own_rows
    net_sub = lax.broadcasted_iota(jnp.int32, (net_count, paths), 0)

    def own(h):
        for t, (at, width) in enumerate(tiles):
            arrive(stage2(h, t, width))
            cols = pl.ds(at, width)
            total_a = st[h, 0, y, :, cols].astype(F32)
            total_b = st[h, 1, x, :, cols].astype(F32)
            for d in range(OTHERS):
                total_a += recv2[h, 0, d, :, cols].astype(F32)
                total_b += recv2[h, 1, d, :, cols].astype(F32)
            SF[0:quarter, cols] = total_a
            SF[quarter:own_rows, cols] = total_b
        summed = SF[...]
        s_high = summed.astype(BF16)
        s_low = (summed - s_high.astype(F32)).astype(BF16)
        both = dot(jnp.concatenate([s_high, s_low], axis=0), Chi[...], NN)
        coupled = both[0:own_rows] + both[own_rows:] + dot(s_high, Clo[...], NN)
        margin = jnp.sqrt(jnp.sum(summed * coupled, axis=1, keepdims=True) + EPSILON)
        own_net = h * half_nets + me // per_net
        cot_row = jnp.sum(jnp.where(net_sub == own_net, cot[...], 0.0), axis=0, keepdims=True)
        cot_column = jnp.sum(jnp.where(mine, cot_row, 0.0), axis=1, keepdims=True)
        grad = ((cot_column / margin) * coupled).astype(BF16)
        G[h, y, x, :, :, 0:bucket_count] = grad.reshape(2, quarter, bucket_count)
        for t in reversed(range(steps)):
            start(gather1(h, t, tiles[t][1]))
        margin_row = jnp.sum(jnp.where(mine, margin, 0.0), axis=0, keepdims=True)
        return jnp.where(net_sub == own_net, margin_row, 0.0)

    def spread(h, chosen):
        for t in chosen:
            arrive(gather1(h, t, tiles[t][1]))
            start(gather2(h, t, tiles[t][1]))

    order = list(reversed(range(steps)))

    early_margins = own(0)
    for i in range(total_steps - LAG, total_steps):
        h, t = i // steps, i % steps
        pass_on(h, t, tiles[t][1])
    spread(0, order[:AHEAD])
    late_margins = own(1)
    spread(0, order[AHEAD:])
    m_send[...] = early_margins + late_margins

    def margin_copies():
        for d in range(1, groups):
            yield pltpu.make_async_remote_copy(
                src_ref=m_send,
                dst_ref=m_recv.at[d - 1],
                send_sem=ms_sems.at[d - 1],
                recv_sem=mr_sems.at[d - 1],
                device_id={"trade": (me + d) % groups},
                device_id_type=MESH,
            )

    start(margin_copies())

    def mean_copies():
        for d in range(1, slabs):
            yield pltpu.make_async_remote_copy(
                src_ref=e_send,
                dst_ref=e_recv.at[d - 1],
                send_sem=es_sems.at[d - 1],
                recv_sem=er_sems.at[d - 1],
                device_id={"path": (slab + d) % slabs},
                device_id_type=MESH,
            )

    def margins():
        arrive(margin_copies())
        all_margins = m_send[...]
        for d in range(groups - 1):
            all_margins += m_recv[d]
        margin_o[...] = all_margins
        my_sum = jnp.sum(all_margins * pw[...], axis=1, keepdims=True)
        e_send[...] = jnp.broadcast_to(my_sum, e_send.shape)
        start(mean_copies())

    def backward(i, carry):
        h, t = i // steps, last - i % steps

        @pl.when(i == SPREAD_AT)
        def _():
            spread(1, order)

        by_width(h * steps + t, lambda h, t, width: arrive(gather2(h, t, width)))
        at = pl.multiple_of(t * TILE, TILE)

        def one(i, carry):
            part = pl.ds(pl.multiple_of(i * STEP, STEP), STEP)
            all_grad = G[h, :, :, :, :, pl.ds(at, TILE)].reshape(half_rows, TILE)
            looked_up = dot(all_grad, hot[pl.ds(at, TILE), part], NN)
            net = nets[:, part]
            total = acc[:, part]
            for n in range(half_nets):
                total += jnp.where(net == h * half_nets + n, looked_up[n * paths : (n + 1) * paths], 0.0)
            acc[:, part] = total
            return carry

        lax.fori_loop(0, capacity // STEP, one, carry, unroll=2)

        @pl.when(i == MARGINS_AT)
        def _():
            margins()

        return carry

    lax.fori_loop(0, total_steps, backward, 0)
    grad_o[...] = (acc[...] * weight[...]).astype(BF16)

    arrive(mean_copies())
    everyone = e_send[...]
    for d in range(slabs - 1):
        everyone += e_recv[d]
    expected_o[...] = everyone / (paths * slabs)

    for h in range(HALVES):
        for t, (at, width) in enumerate(tiles):
            for stage in (stage1, stage2, gather1, gather2):
                for copy in stage(h, t, width):
                    copy.wait_send()
    for copy in (*margin_copies(), *mean_copies()):
        copy.wait_send()


def finish(grad, margin, expected, grad_o, margin_o, expected_o):
    block = grad_o.shape[0]
    at = pl.multiple_of(pl.program_id(0) * block, block)
    grad_o[...] = grad[:, pl.ds(at, block)].T
    margin_o[...] = margin[...]
    net_count = margin.shape[0]
    sub = lax.broadcasted_iota(jnp.int32, margin.shape, 0)
    lane = lax.broadcasted_iota(jnp.int32, margin.shape, 1)
    row = jnp.sum(jnp.where(sub == lane, expected[...], 0.0), axis=0, keepdims=True)
    expected_o[...] = row[:, 0:net_count]


def shards(groups, slabs, deltas, net_ids, block_ids, bucket_map, risk_weight, counts, correlation, path_weight, margin_cotangent):
    capacity, paths = deltas.shape
    buckets = correlation.shape[0]
    net_count = margin_cotangent.shape[0]
    rows = net_count * paths
    half = rows // HALVES // groups // 2
    tile_count = len(tiles_of(buckets))
    padded = tile_count * TILE
    vmem = pl.BlockSpec(memory_space=pltpu.VMEM)
    smem = pl.BlockSpec(memory_space=pltpu.SMEM)
    dma = pltpu.SemaphoreType.DMA
    anywhere = pl.BlockSpec(memory_space=pltpu.HBM)
    in_hbm = functools.partial(pltpu.with_memory_space_constraint, memory_space=pltpu.HBM)
    margin, expected, turned_grad = pl.pallas_call(
        functools.partial(kernel, groups, slabs),
        out_shape=(
            jax.ShapeDtypeStruct((net_count, paths), F32),
            jax.ShapeDtypeStruct((net_count, paths), F32),
            jax.ShapeDtypeStruct((paths, capacity), BF16),
        ),
        in_specs=[anywhere] * 5 + [smem] + [anywhere] * 3,
        out_specs=(vmem, vmem, vmem),
        scratch_shapes=[
            pltpu.VMEM((capacity, paths), BF16),
            pltpu.VMEM((1, capacity), jnp.int32),
            pltpu.VMEM((1, capacity), jnp.int32),
            pltpu.VMEM((risk_weight.size // LANES, LANES), F32),
            pltpu.VMEM((bucket_map.size // LANES, LANES), jnp.int32),
            pltpu.VMEM((1, paths), F32),
            pltpu.VMEM((net_count, paths), F32),
            pltpu.VMEM((1, capacity), F32),
            pltpu.VMEM((4 * LANES, LANES), BF16),
            pltpu.VMEM((padded, capacity), BF16),
            pltpu.VMEM((rows, capacity), BF16),
            pltpu.VMEM((1, capacity), F32),
            pltpu.VMEM((HALVES, SIDE, SIDE, 2, half, padded), BF16),
            pltpu.VMEM((HALVES, 2, OTHERS, SIDE, half, buckets), BF16),
            pltpu.VMEM((HALVES, 2, SIDE, half, buckets), BF16),
            pltpu.VMEM((HALVES, 2, OTHERS, half, buckets), BF16),
            pltpu.VMEM((2 * half, buckets), F32),
            pltpu.VMEM((buckets, buckets), F32),
            pltpu.VMEM((buckets, buckets), BF16),
            pltpu.VMEM((buckets, buckets), BF16),
            pltpu.VMEM((HALVES, SIDE, SIDE, 2, half, padded), BF16),
            pltpu.VMEM((paths, capacity), F32),
            pltpu.VMEM((net_count, paths), F32),
            pltpu.VMEM((groups - 1, net_count, paths), F32),
            pltpu.VMEM((net_count, paths), F32),
            pltpu.VMEM((slabs - 1, net_count, paths), F32),
            dma,
            dma((7,)),
            dma((8, HALVES * tile_count, OTHERS)),
            dma((8, HALVES * tile_count, OTHERS)),
            dma((groups - 1,)),
            dma((groups - 1,)),
            dma((slabs - 1,)),
            dma((slabs - 1,)),
        ],
        compiler_params=pltpu.CompilerParams(
            collective_id=0, has_side_effects=True, vmem_limit_bytes=52 * 1024 * 1024
        ),
        name="margin_exchange",
    )(
        in_hbm(deltas),
        in_hbm(net_ids.reshape(1, capacity)),
        in_hbm(block_ids.reshape(1, capacity)),
        in_hbm(risk_weight.reshape(-1, LANES)),
        in_hbm(bucket_map.reshape(-1, LANES)),
        counts,
        in_hbm(correlation),
        in_hbm(path_weight.reshape(1, paths)),
        in_hbm(margin_cotangent),
    )
    block = capacity // 2
    whole = pl.BlockSpec((net_count, paths), lambda i: (0, 0))
    trade_grad, margin, expected = pl.pallas_call(
        finish,
        grid=(capacity // block,),
        out_shape=(
            jax.ShapeDtypeStruct((capacity, paths), BF16),
            jax.ShapeDtypeStruct((net_count, paths), F32),
            jax.ShapeDtypeStruct((1, net_count), F32),
        ),
        in_specs=[vmem, vmem, vmem],
        out_specs=(
            pl.BlockSpec((block, paths), lambda i: (i, 0)),
            whole,
            pl.BlockSpec((1, net_count), lambda i: (0, 0)),
        ),
        compiler_params=pltpu.CompilerParams(vmem_limit_bytes=8 * 1024 * 1024),
        name="finish",
    )(turned_grad, margin, expected)
    return margin, expected.reshape(net_count), trade_grad


def solution(mesh):
    placed = (
        P("trade", "path"),
        P("trade"),
        P("trade"),
        P(),
        P(),
        P("trade"),
        P(),
        P("path"),
        P(None, "path"),
    )
    return jax.shard_map(
        functools.partial(shards, mesh.shape["trade"], mesh.shape["path"]),
        mesh=mesh,
        in_specs=placed,
        out_specs=(P(None, "path"), P(), P("trade", "path")),
        check_vma=False,
    )
```

```python
import functools

import jax
import jax.numpy as jnp
from jax import lax
from jax.experimental import pallas as pl
from jax.experimental.pallas import tpu as pltpu
from jax.sharding import PartitionSpec as P

EPSILON = 1e-06
LANES = 128
F32 = jnp.float32
BF16 = jnp.bfloat16
MESH = pl.DeviceIdType.MESH
SIDE = 4
OTHERS = SIDE - 1
CHUNK = 512
NT = (((1,), (1,)), ((), ()))
NN = (((1,), (0,)), ((), ()))
TN = (((0,), (0,)), ((), ()))


def dot(a, b, dims):
    return lax.dot_general(a, b, dims, preferred_element_type=F32)


TILE = 256
HALVES = 2
LAG = 3
STEP = 2048
AHEAD = 3
SPREAD_AT = 2
MARGINS_AT = 5


def tiles_of(total):
    cuts, at = [], 0
    while at < total:
        width = min(TILE, total - at)
        cuts.append((at, width))
        at += width
    return cuts


def kernel(
    groups,
    slabs,
    deltas_in,
    nets_in,
    blocks_in,
    rw_in,
    bm_in,
    counts,
    corr,
    pw_in,
    cot_in,
    margin_o,
    expected_o,
    grad_o,
    slots,
    nets,
    blocks,
    rw,
    bm,
    pw,
    cot,
    weight,
    table,
    hot,
    X,
    wrow,
    S,
    recv1,
    st,
    recv2,
    SF,
    C,
    Chi,
    Clo,
    G,
    acc,
    m_send,
    m_recv,
    e_send,
    e_recv,
    c_sem,
    in_sems,
    s_sems,
    r_sems,
    ms_sems,
    mr_sems,
    es_sems,
    er_sems,
):
    me = lax.axis_index("trade")
    slab = lax.axis_index("path")
    y, x = me // SIDE, me % SIDE
    capacity = slots.shape[0]
    bucket_count = corr.shape[0]
    net_count, paths = cot.shape
    rows = net_count * paths
    half_rows = rows // HALVES
    half_nets = net_count // HALVES
    own_rows = half_rows // groups
    quarter = own_rows // 2
    tiles = tiles_of(bucket_count)

    entering = [
        pltpu.make_async_copy(source, target, in_sems.at[i])
        for i, (source, target) in enumerate(
            (
                (rw_in, rw),
                (bm_in, bm),
                (blocks_in, blocks),
                (nets_in, nets),
                (deltas_in, slots),
                (pw_in, pw),
                (cot_in, cot),
            )
        )
    ]
    for copy in entering:
        copy.start()
    c_copy = pltpu.make_async_copy(corr, C, c_sem)

    barrier = pltpu.get_barrier_semaphore()
    for d in range(1, groups):
        pl.semaphore_signal(barrier, inc=1, device_id={"trade": (me + d) % groups}, device_id_type=MESH)
    for d in range(1, slabs):
        pl.semaphore_signal(barrier, inc=1, device_id={"path": (slab + d) % slabs}, device_id_type=MESH)

    table[...] = jnp.zeros_like(table)
    for copy in entering:
        copy.wait()
    c_copy.start()
    table_rows = rw.shape[0]
    w_all = rw[...]
    w1 = w_all.astype(BF16).astype(F32)
    b_all = bm[...]
    parts = (w1, w_all - w1, (b_all // LANES).astype(F32), (b_all % LANES).astype(F32))
    for k, part in enumerate(parts):
        table[k * LANES : (k + 1) * LANES, 0:table_rows] = part.T.astype(BF16)
    live_count = counts[0]

    def look_up(i, carry):
        at = pl.multiple_of(i * CHUNK, CHUNK)
        ids = blocks[:, pl.ds(at, CHUNK)]
        high, low = ids // LANES, ids % LANES
        sub = lax.broadcasted_iota(jnp.int32, (LANES, CHUNK), 0)
        pick = jnp.where(sub == high, 1.0, 0.0).astype(BF16)
        found = dot(table[...], pick, NN)
        keep = sub == low
        parts = [
            jnp.sum(jnp.where(keep, found[k * LANES : (k + 1) * LANES], 0.0), axis=0, keepdims=True)
            for k in range(4)
        ]
        slot = at + lax.broadcasted_iota(jnp.int32, (1, CHUNK), 1)
        w = jnp.where(slot < live_count, parts[0] + parts[1], 0.0)
        weight[:, pl.ds(at, CHUNK)] = w
        wrow[:, pl.ds(at, CHUNK)] = parts[2] * LANES + parts[3]
        turned = slots[pl.ds(at, CHUNK), :].T.astype(F32)
        weighted = turned * w
        net = nets[:, pl.ds(at, CHUNK)]
        for n in range(net_count):
            X[n * paths : (n + 1) * paths, pl.ds(at, CHUNK)] = jnp.where(net == n, weighted, 0.0).astype(BF16)
        return carry

    lax.fori_loop(0, capacity // CHUNK, look_up, 0, unroll=4)

    def remote(src, dst, phase, tile, d, peer):
        return pltpu.make_async_remote_copy(
            src_ref=src,
            dst_ref=dst,
            send_sem=s_sems.at[phase, tile, d - 1],
            recv_sem=r_sems.at[phase, tile, d - 1],
            device_id={"trade": peer},
            device_id_type=MESH,
        )

    def mates(d):
        kx, ky = (x + d) % SIDE, (y + d) % SIDE
        return kx, ky, y * SIDE + kx, ky * SIDE + x

    def columns(t, width):
        at = t * TILE
        return pl.ds(at if isinstance(at, int) else pl.multiple_of(at, TILE), width)

    steps = len(tiles)
    last = steps - 1
    last_width = tiles[last][1]

    def stage1(h, t, width):
        cols, i = columns(t, width), h * steps + t
        for d in (2, 1, 3):
            kx, ky, in_row, in_column = mates(d)
            yield remote(S.at[h, :, kx, 0, :, cols], recv1.at[h, 0, d - 1, :, :, cols], 0, i, d, in_row)
            yield remote(S.at[h, ky, :, 1, :, cols], recv1.at[h, 1, d - 1, :, :, cols], 1, i, d, in_column)

    def stage2(h, t, width):
        cols, i = columns(t, width), h * steps + t
        for d in (2, 1, 3):
            kx, ky, in_row, in_column = mates(d)
            yield remote(st.at[h, 0, ky, :, cols], recv2.at[h, 0, d - 1, :, cols], 2, i, d, in_column)
            yield remote(st.at[h, 1, kx, :, cols], recv2.at[h, 1, d - 1, :, cols], 3, i, d, in_row)

    def gather1(h, t, width):
        cols, i = columns(t, width), h * steps + t
        own_a, own_b = G.at[h, y, x, 0, :, cols], G.at[h, y, x, 1, :, cols]
        for d in (2, 1, 3):
            kx, ky, in_row, in_column = mates(d)
            yield remote(own_a, own_a, 4, i, d, in_column)
            yield remote(own_b, own_b, 5, i, d, in_row)

    def gather2(h, t, width):
        cols, i = columns(t, width), h * steps + t
        all_a, all_b = G.at[h, :, x, 0, :, cols], G.at[h, y, :, 1, :, cols]
        for d in (2, 1, 3):
            kx, ky, in_row, in_column = mates(d)
            yield remote(all_a, all_a, 6, i, d, in_row)
            yield remote(all_b, all_b, 7, i, d, in_column)

    def start(copies):
        for copy in copies:
            copy.start()

    def arrive(copies):
        for copy in copies:
            copy.wait_recv()

    def by_width(i, run):
        h, t = i // steps, i % steps

        @pl.when(t < last)
        def _():
            run(h, t, TILE)

        @pl.when(t == last)
        def _():
            run(h, last, last_width)

    def pass_on(h, t, width):
        arrive(stage1(h, t, width))
        cols = columns(t, width)
        total_a = S[h, :, x, 0, :, cols].astype(F32)
        total_b = S[h, y, :, 1, :, cols].astype(F32)
        for d in range(OTHERS):
            total_a += recv1[h, 0, d, :, :, cols].astype(F32)
            total_b += recv1[h, 1, d, :, :, cols].astype(F32)
        st[h, 0, :, :, cols] = total_a.astype(BF16)
        st[h, 1, :, :, cols] = total_b.astype(BF16)
        start(stage2(h, t, width))

    def forward(i, carry):
        h, t = i // steps, i % steps
        at = pl.multiple_of(t * TILE, TILE)

        @pl.when(h == 0)
        def _():
            for k in range(capacity // CHUNK):
                part = pl.ds(k * CHUNK, CHUNK)
                bucket = wrow[:, part]
                sub = (at + lax.broadcasted_iota(jnp.int32, (TILE, CHUNK), 0)).astype(F32)
                hot[pl.ds(at, TILE), part] = jnp.where(sub == bucket, 1.0, 0.0).astype(BF16)

        half = pl.ds(pl.multiple_of(h * half_rows, half_rows), half_rows)
        result = dot(X[half, :], hot[pl.ds(at, TILE), :], NT).astype(BF16)
        S[h, :, :, :, :, pl.ds(at, TILE)] = result.reshape(S.shape[1:-1] + (TILE,))

        @pl.when(i == 0)
        def _():
            pl.semaphore_wait(barrier, groups - 1 + slabs - 1)

        by_width(i, lambda h, t, width: start(stage1(h, t, width)))

        @pl.when(i >= LAG)
        def _():
            by_width(i - LAG, pass_on)

        return carry

    total_steps = HALVES * steps
    lax.fori_loop(0, total_steps, forward, 0)
    c_copy.wait()
    for at, width in tiles:
        block = C[:, at : at + width]
        high = block.astype(BF16)
        Chi[:, at : at + width] = high
        Clo[:, at : at + width] = (block - high.astype(F32)).astype(BF16)

    per_net = paths // own_rows
    own_part = me % per_net
    sub = lax.broadcasted_iota(jnp.int32, (own_rows, paths), 0)
    lane = lax.broadcasted_iota(jnp.int32, (own_rows, paths), 1)
    mine = lane == sub + own_part * own_rows
    net_sub = lax.broadcasted_iota(jnp.int32, (net_count, paths), 0)

    def own(h):
        for t, (at, width) in enumerate(tiles):
            arrive(stage2(h, t, width))
            cols = pl.ds(at, width)
            total_a = st[h, 0, y, :, cols].astype(F32)
            total_b = st[h, 1, x, :, cols].astype(F32)
            for d in range(OTHERS):
                total_a += recv2[h, 0, d, :, cols].astype(F32)
                total_b += recv2[h, 1, d, :, cols].astype(F32)
            SF[0:quarter, cols] = total_a
            SF[quarter:own_rows, cols] = total_b
        summed = SF[...]
        s_high = summed.astype(BF16)
        s_low = (summed - s_high.astype(F32)).astype(BF16)
        both = dot(jnp.concatenate([s_high, s_low], axis=0), Chi[...], NN)
        coupled = both[0:own_rows] + both[own_rows:] + dot(s_high, Clo[...], NN)
        margin = jnp.sqrt(jnp.sum(summed * coupled, axis=1, keepdims=True) + EPSILON)
        own_net = h * half_nets + me // per_net
        cot_row = jnp.sum(jnp.where(net_sub == own_net, cot[...], 0.0), axis=0, keepdims=True)
        cot_column = jnp.sum(jnp.where(mine, cot_row, 0.0), axis=1, keepdims=True)
        grad = ((cot_column / margin) * coupled).astype(BF16)
        G[h, y, x, :, :, 0:bucket_count] = grad.reshape(2, quarter, bucket_count)
        for t in reversed(range(steps)):
            start(gather1(h, t, tiles[t][1]))
        margin_row = jnp.sum(jnp.where(mine, margin, 0.0), axis=0, keepdims=True)
        return jnp.where(net_sub == own_net, margin_row, 0.0)

    def spread(h, chosen):
        for t in chosen:
            arrive(gather1(h, t, tiles[t][1]))
            start(gather2(h, t, tiles[t][1]))

    order = list(reversed(range(steps)))

    early_margins = own(0)
    acc[...] = jnp.zeros_like(acc)
    padded = hot.shape[0]
    if padded > bucket_count:
        G[:, :, :, :, :, bucket_count:padded] = jnp.zeros(G.shape[:-1] + (padded - bucket_count,), BF16)
    for i in range(total_steps - LAG, total_steps):
        h, t = i // steps, i % steps
        pass_on(h, t, tiles[t][1])
    spread(0, order[:AHEAD])
    late_margins = own(1)
    spread(0, order[AHEAD:])
    m_send[...] = early_margins + late_margins

    def margin_copies():
        for d in range(1, groups):
            yield pltpu.make_async_remote_copy(
                src_ref=m_send,
                dst_ref=m_recv.at[d - 1],
                send_sem=ms_sems.at[d - 1],
                recv_sem=mr_sems.at[d - 1],
                device_id={"trade": (me + d) % groups},
                device_id_type=MESH,
            )

    start(margin_copies())

    def mean_copies():
        for d in range(1, slabs):
            yield pltpu.make_async_remote_copy(
                src_ref=e_send,
                dst_ref=e_recv.at[d - 1],
                send_sem=es_sems.at[d - 1],
                recv_sem=er_sems.at[d - 1],
                device_id={"path": (slab + d) % slabs},
                device_id_type=MESH,
            )

    def margins():
        arrive(margin_copies())
        all_margins = m_send[...]
        for d in range(groups - 1):
            all_margins += m_recv[d]
        margin_o[...] = all_margins
        my_sum = jnp.sum(all_margins * pw[...], axis=1, keepdims=True)
        e_send[...] = jnp.broadcast_to(my_sum, e_send.shape)
        start(mean_copies())

    def backward(i, carry):
        h, t = i // steps, last - i % steps

        @pl.when(i == SPREAD_AT)
        def _():
            spread(1, order)

        by_width(h * steps + t, lambda h, t, width: arrive(gather2(h, t, width)))
        at = pl.multiple_of(t * TILE, TILE)

        def one(i, carry):
            part = pl.ds(pl.multiple_of(i * STEP, STEP), STEP)
            all_grad = G[h, :, :, :, :, pl.ds(at, TILE)].reshape(half_rows, TILE)
            looked_up = dot(all_grad, hot[pl.ds(at, TILE), part], NN)
            net = nets[:, part]
            total = acc[:, part]
            for n in range(half_nets):
                total += jnp.where(net == h * half_nets + n, looked_up[n * paths : (n + 1) * paths], 0.0)
            acc[:, part] = total
            return carry

        lax.fori_loop(0, capacity // STEP, one, carry, unroll=2)

        @pl.when(i == MARGINS_AT)
        def _():
            margins()

        return carry

    lax.fori_loop(0, total_steps, backward, 0)
    grad_o[...] = (acc[...] * weight[...]).astype(BF16)

    arrive(mean_copies())
    everyone = e_send[...]
    for d in range(slabs - 1):
        everyone += e_recv[d]
    expected_o[...] = everyone / (paths * slabs)

    for h in range(HALVES):
        for t, (at, width) in enumerate(tiles):
            for stage in (stage1, stage2, gather1, gather2):
                for copy in stage(h, t, width):
                    copy.wait_send()
    for copy in (*margin_copies(), *mean_copies()):
        copy.wait_send()


def finish(grad, margin, expected, grad_o, margin_o, expected_o):
    block = grad_o.shape[0]
    at = pl.multiple_of(pl.program_id(0) * block, block)
    grad_o[...] = grad[:, pl.ds(at, block)].T
    margin_o[...] = margin[...]
    net_count = margin.shape[0]
    sub = lax.broadcasted_iota(jnp.int32, margin.shape, 0)
    lane = lax.broadcasted_iota(jnp.int32, margin.shape, 1)
    row = jnp.sum(jnp.where(sub == lane, expected[...], 0.0), axis=0, keepdims=True)
    expected_o[...] = row[:, 0:net_count]


def shards(groups, slabs, deltas, net_ids, block_ids, bucket_map, risk_weight, counts, correlation, path_weight, margin_cotangent):
    capacity, paths = deltas.shape
    buckets = correlation.shape[0]
    net_count = margin_cotangent.shape[0]
    rows = net_count * paths
    half = rows // HALVES // groups // 2
    tile_count = len(tiles_of(buckets))
    padded = tile_count * TILE
    vmem = pl.BlockSpec(memory_space=pltpu.VMEM)
    smem = pl.BlockSpec(memory_space=pltpu.SMEM)
    dma = pltpu.SemaphoreType.DMA
    anywhere = pl.BlockSpec(memory_space=pltpu.HBM)
    in_hbm = functools.partial(pltpu.with_memory_space_constraint, memory_space=pltpu.HBM)
    margin, expected, turned_grad = pl.pallas_call(
        functools.partial(kernel, groups, slabs),
        out_shape=(
            jax.ShapeDtypeStruct((net_count, paths), F32),
            jax.ShapeDtypeStruct((net_count, paths), F32),
            jax.ShapeDtypeStruct((paths, capacity), BF16),
        ),
        in_specs=[anywhere] * 5 + [smem] + [anywhere] * 3,
        out_specs=(vmem, vmem, vmem),
        scratch_shapes=[
            pltpu.VMEM((capacity, paths), BF16),
            pltpu.VMEM((1, capacity), jnp.int32),
            pltpu.VMEM((1, capacity), jnp.int32),
            pltpu.VMEM((risk_weight.size // LANES, LANES), F32),
            pltpu.VMEM((bucket_map.size // LANES, LANES), jnp.int32),
            pltpu.VMEM((1, paths), F32),
            pltpu.VMEM((net_count, paths), F32),
            pltpu.VMEM((1, capacity), F32),
            pltpu.VMEM((4 * LANES, LANES), BF16),
            pltpu.VMEM((padded, capacity), BF16),
            pltpu.VMEM((rows, capacity), BF16),
            pltpu.VMEM((1, capacity), F32),
            pltpu.VMEM((HALVES, SIDE, SIDE, 2, half, padded), BF16),
            pltpu.VMEM((HALVES, 2, OTHERS, SIDE, half, buckets), BF16),
            pltpu.VMEM((HALVES, 2, SIDE, half, buckets), BF16),
            pltpu.VMEM((HALVES, 2, OTHERS, half, buckets), BF16),
            pltpu.VMEM((2 * half, buckets), F32),
            pltpu.VMEM((buckets, buckets), F32),
            pltpu.VMEM((buckets, buckets), BF16),
            pltpu.VMEM((buckets, buckets), BF16),
            pltpu.VMEM((HALVES, SIDE, SIDE, 2, half, padded), BF16),
            pltpu.VMEM((paths, capacity), F32),
            pltpu.VMEM((net_count, paths), F32),
            pltpu.VMEM((groups - 1, net_count, paths), F32),
            pltpu.VMEM((net_count, paths), F32),
            pltpu.VMEM((slabs - 1, net_count, paths), F32),
            dma,
            dma((7,)),
            dma((8, HALVES * tile_count, OTHERS)),
            dma((8, HALVES * tile_count, OTHERS)),
            dma((groups - 1,)),
            dma((groups - 1,)),
            dma((slabs - 1,)),
            dma((slabs - 1,)),
        ],
        compiler_params=pltpu.CompilerParams(
            collective_id=0, has_side_effects=True, vmem_limit_bytes=52 * 1024 * 1024
        ),
        name="margin_exchange",
    )(
        in_hbm(deltas),
        in_hbm(net_ids.reshape(1, capacity)),
        in_hbm(block_ids.reshape(1, capacity)),
        in_hbm(risk_weight.reshape(-1, LANES)),
        in_hbm(bucket_map.reshape(-1, LANES)),
        counts,
        in_hbm(correlation),
        in_hbm(path_weight.reshape(1, paths)),
        in_hbm(margin_cotangent),
    )
    block = capacity // 2
    whole = pl.BlockSpec((net_count, paths), lambda i: (0, 0))
    trade_grad, margin, expected = pl.pallas_call(
        finish,
        grid=(capacity // block,),
        out_shape=(
            jax.ShapeDtypeStruct((capacity, paths), BF16),
            jax.ShapeDtypeStruct((net_count, paths), F32),
            jax.ShapeDtypeStruct((1, net_count), F32),
        ),
        in_specs=[vmem, vmem, vmem],
        out_specs=(
            pl.BlockSpec((block, paths), lambda i: (i, 0)),
            whole,
            pl.BlockSpec((1, net_count), lambda i: (0, 0)),
        ),
        compiler_params=pltpu.CompilerParams(vmem_limit_bytes=8 * 1024 * 1024),
        name="finish",
    )(turned_grad, margin, expected)
    return margin, expected.reshape(net_count), trade_grad


def solution(mesh):
    placed = (
        P("trade", "path"),
        P("trade"),
        P("trade"),
        P(),
        P(),
        P("trade"),
        P(),
        P("path"),
        P(None, "path"),
    )
    return jax.shard_map(
        functools.partial(shards, mesh.shape["trade"], mesh.shape["path"]),
        mesh=mesh,
        in_specs=placed,
        out_specs=(P(None, "path"), P(), P("trade", "path")),
        check_vma=False,
    )
```

```python
import functools

import jax
import jax.numpy as jnp
from jax import lax
from jax.experimental import pallas as pl
from jax.experimental.pallas import tpu as pltpu
from jax.sharding import PartitionSpec as P

EPSILON = 1e-06
LANES = 128
F32 = jnp.float32
BF16 = jnp.bfloat16
MESH = pl.DeviceIdType.MESH
SIDE = 4
OTHERS = SIDE - 1
CHUNK = 512
NT = (((1,), (1,)), ((), ()))
NN = (((1,), (0,)), ((), ()))
TN = (((0,), (0,)), ((), ()))


def dot(a, b, dims):
    return lax.dot_general(a, b, dims, preferred_element_type=F32)


TILE = 256
HALVES = 2
LAG = 3
STEP = 2048
AHEAD = 3
SPREAD_AT = 2
MARGINS_AT = 5


def tiles_of(total):
    cuts, at = [], 0
    while at < total:
        width = min(TILE, total - at)
        cuts.append((at, width))
        at += width
    return cuts


def kernel(
    groups,
    slabs,
    deltas_in,
    nets_in,
    blocks_in,
    rw_in,
    bm_in,
    counts,
    corr,
    pw_in,
    cot_in,
    margin_o,
    expected_o,
    grad_o,
    slots,
    nets,
    blocks,
    rw,
    bm,
    pw,
    cot,
    weight,
    table,
    hot,
    X,
    wrow,
    S,
    recv1,
    st,
    recv2,
    SF,
    C,
    Chi,
    Clo,
    G,
    acc,
    m_send,
    m_recv,
    e_send,
    e_recv,
    c_sem,
    in_sems,
    s_sems,
    r_sems,
    ms_sems,
    mr_sems,
    es_sems,
    er_sems,
):
    me = lax.axis_index("trade")
    slab = lax.axis_index("path")
    y, x = me // SIDE, me % SIDE
    capacity = slots.shape[0]
    bucket_count = corr.shape[0]
    net_count, paths = cot.shape
    rows = net_count * paths
    half_rows = rows // HALVES
    half_nets = net_count // HALVES
    own_rows = half_rows // groups
    quarter = own_rows // 2
    tiles = tiles_of(bucket_count)

    entering = [
        pltpu.make_async_copy(source, target, in_sems.at[i])
        for i, (source, target) in enumerate(
            (
                (rw_in, rw),
                (bm_in, bm),
                (blocks_in, blocks),
                (nets_in, nets),
                (deltas_in, slots),
                (pw_in, pw),
                (cot_in, cot),
            )
        )
    ]
    for copy in entering:
        copy.start()
    c_copy = pltpu.make_async_copy(corr, C, c_sem)

    barrier = pltpu.get_barrier_semaphore()
    for d in range(1, groups):
        pl.semaphore_signal(barrier, inc=1, device_id={"trade": (me + d) % groups}, device_id_type=MESH)
    for d in range(1, slabs):
        pl.semaphore_signal(barrier, inc=1, device_id={"path": (slab + d) % slabs}, device_id_type=MESH)

    table[...] = jnp.zeros_like(table)
    for copy in entering:
        copy.wait()
    c_copy.start()
    table_rows = rw.shape[0]
    w_all = rw[...]
    w1 = w_all.astype(BF16).astype(F32)
    b_all = bm[...]
    parts = (w1, w_all - w1, (b_all // LANES).astype(F32), (b_all % LANES).astype(F32))
    for k, part in enumerate(parts):
        table[k * LANES : (k + 1) * LANES, 0:table_rows] = part.T.astype(BF16)
    live_count = counts[0]

    def look_up(i, carry):
        at = pl.multiple_of(i * CHUNK, CHUNK)
        ids = blocks[:, pl.ds(at, CHUNK)]
        high, low = ids // LANES, ids % LANES
        sub = lax.broadcasted_iota(jnp.int32, (LANES, CHUNK), 0)
        pick = jnp.where(sub == high, 1.0, 0.0).astype(BF16)
        keep = sub == low
        parts = [
            jnp.sum(
                jnp.where(keep, dot(table[k * LANES : (k + 1) * LANES], pick, NN), 0.0), axis=0, keepdims=True
            )
            for k in range(4)
        ]
        slot = at + lax.broadcasted_iota(jnp.int32, (1, CHUNK), 1)
        w = jnp.where(slot < live_count, parts[0] + parts[1], 0.0)
        weight[:, pl.ds(at, CHUNK)] = w
        wrow[:, pl.ds(at, CHUNK)] = parts[2] * LANES + parts[3]
        turned = slots[pl.ds(at, CHUNK), :].T.astype(F32)
        weighted = turned * w
        net = nets[:, pl.ds(at, CHUNK)]
        for n in range(net_count):
            X[n * paths : (n + 1) * paths, pl.ds(at, CHUNK)] = jnp.where(net == n, weighted, 0.0).astype(BF16)
        return carry

    lax.fori_loop(0, capacity // CHUNK, look_up, 0, unroll=4)

    def remote(src, dst, phase, tile, d, peer):
        return pltpu.make_async_remote_copy(
            src_ref=src,
            dst_ref=dst,
            send_sem=s_sems.at[phase, tile, d - 1],
            recv_sem=r_sems.at[phase, tile, d - 1],
            device_id={"trade": peer},
            device_id_type=MESH,
        )

    def mates(d):
        kx, ky = (x + d) % SIDE, (y + d) % SIDE
        return kx, ky, y * SIDE + kx, ky * SIDE + x

    def columns(t, width):
        at = t * TILE
        return pl.ds(at if isinstance(at, int) else pl.multiple_of(at, TILE), width)

    steps = len(tiles)
    last = steps - 1
    last_width = tiles[last][1]

    def stage1(h, t, width):
        cols, i = columns(t, width), h * steps + t
        for d in (2, 1, 3):
            kx, ky, in_row, in_column = mates(d)
            yield remote(S.at[h, :, kx, 0, :, cols], recv1.at[h, 0, d - 1, :, :, cols], 0, i, d, in_row)
            yield remote(S.at[h, ky, :, 1, :, cols], recv1.at[h, 1, d - 1, :, :, cols], 1, i, d, in_column)

    def stage2(h, t, width):
        cols, i = columns(t, width), h * steps + t
        for d in (2, 1, 3):
            kx, ky, in_row, in_column = mates(d)
            yield remote(st.at[h, 0, ky, :, cols], recv2.at[h, 0, d - 1, :, cols], 2, i, d, in_column)
            yield remote(st.at[h, 1, kx, :, cols], recv2.at[h, 1, d - 1, :, cols], 3, i, d, in_row)

    def gather1(h, t, width):
        cols, i = columns(t, width), h * steps + t
        own_a, own_b = G.at[h, y, x, 0, :, cols], G.at[h, y, x, 1, :, cols]
        for d in (2, 1, 3):
            kx, ky, in_row, in_column = mates(d)
            yield remote(own_a, own_a, 4, i, d, in_column)
            yield remote(own_b, own_b, 5, i, d, in_row)

    def gather2(h, t, width):
        cols, i = columns(t, width), h * steps + t
        all_a, all_b = G.at[h, :, x, 0, :, cols], G.at[h, y, :, 1, :, cols]
        for d in (2, 1, 3):
            kx, ky, in_row, in_column = mates(d)
            yield remote(all_a, all_a, 6, i, d, in_row)
            yield remote(all_b, all_b, 7, i, d, in_column)

    def start(copies):
        for copy in copies:
            copy.start()

    def arrive(copies):
        for copy in copies:
            copy.wait_recv()

    def by_width(i, run):
        h, t = i // steps, i % steps

        @pl.when(t < last)
        def _():
            run(h, t, TILE)

        @pl.when(t == last)
        def _():
            run(h, last, last_width)

    def pass_on(h, t, width):
        arrive(stage1(h, t, width))
        cols = columns(t, width)
        total_a = S[h, :, x, 0, :, cols].astype(F32)
        total_b = S[h, y, :, 1, :, cols].astype(F32)
        for d in range(OTHERS):
            total_a += recv1[h, 0, d, :, :, cols].astype(F32)
            total_b += recv1[h, 1, d, :, :, cols].astype(F32)
        st[h, 0, :, :, cols] = total_a.astype(BF16)
        st[h, 1, :, :, cols] = total_b.astype(BF16)
        start(stage2(h, t, width))

    def forward(i, carry):
        h, t = i // steps, i % steps
        at = pl.multiple_of(t * TILE, TILE)

        @pl.when(h == 0)
        def _():
            for k in range(capacity // CHUNK):
                part = pl.ds(k * CHUNK, CHUNK)
                bucket = wrow[:, part]
                sub = (at + lax.broadcasted_iota(jnp.int32, (TILE, CHUNK), 0)).astype(F32)
                hot[pl.ds(at, TILE), part] = jnp.where(sub == bucket, 1.0, 0.0).astype(BF16)

        half = pl.ds(pl.multiple_of(h * half_rows, half_rows), half_rows)
        result = dot(X[half, :], hot[pl.ds(at, TILE), :], NT).astype(BF16)
        S[h, :, :, :, :, pl.ds(at, TILE)] = result.reshape(S.shape[1:-1] + (TILE,))

        @pl.when(i == 0)
        def _():
            pl.semaphore_wait(barrier, groups - 1 + slabs - 1)

        by_width(i, lambda h, t, width: start(stage1(h, t, width)))

        @pl.when(i >= LAG)
        def _():
            by_width(i - LAG, pass_on)

        return carry

    total_steps = HALVES * steps
    lax.fori_loop(0, total_steps, forward, 0)
    c_copy.wait()
    for at, width in tiles:
        block = C[:, at : at + width]
        high = block.astype(BF16)
        Chi[:, at : at + width] = high
        Clo[:, at : at + width] = (block - high.astype(F32)).astype(BF16)

    per_net = paths // own_rows
    own_part = me % per_net
    sub = lax.broadcasted_iota(jnp.int32, (own_rows, paths), 0)
    lane = lax.broadcasted_iota(jnp.int32, (own_rows, paths), 1)
    mine = lane == sub + own_part * own_rows
    net_sub = lax.broadcasted_iota(jnp.int32, (net_count, paths), 0)

    def own(h):
        for t, (at, width) in enumerate(tiles):
            arrive(stage2(h, t, width))
            cols = pl.ds(at, width)
            total_a = st[h, 0, y, :, cols].astype(F32)
            total_b = st[h, 1, x, :, cols].astype(F32)
            for d in range(OTHERS):
                total_a += recv2[h, 0, d, :, cols].astype(F32)
                total_b += recv2[h, 1, d, :, cols].astype(F32)
            SF[0:quarter, cols] = total_a
            SF[quarter:own_rows, cols] = total_b
        summed = SF[...]
        s_high = summed.astype(BF16)
        s_low = (summed - s_high.astype(F32)).astype(BF16)
        both = dot(jnp.concatenate([s_high, s_low], axis=0), Chi[...], NN)
        coupled = both[0:own_rows] + both[own_rows:] + dot(s_high, Clo[...], NN)
        margin = jnp.sqrt(jnp.sum(summed * coupled, axis=1, keepdims=True) + EPSILON)
        own_net = h * half_nets + me // per_net
        cot_row = jnp.sum(jnp.where(net_sub == own_net, cot[...], 0.0), axis=0, keepdims=True)
        cot_column = jnp.sum(jnp.where(mine, cot_row, 0.0), axis=1, keepdims=True)
        grad = ((cot_column / margin) * coupled).astype(BF16)
        G[h, y, x, :, :, 0:bucket_count] = grad.reshape(2, quarter, bucket_count)
        for t in reversed(range(steps)):
            start(gather1(h, t, tiles[t][1]))
        margin_row = jnp.sum(jnp.where(mine, margin, 0.0), axis=0, keepdims=True)
        return jnp.where(net_sub == own_net, margin_row, 0.0)

    def spread(h, chosen):
        for t in chosen:
            arrive(gather1(h, t, tiles[t][1]))
            start(gather2(h, t, tiles[t][1]))

    order = list(reversed(range(steps)))

    early_margins = own(0)
    acc[...] = jnp.zeros_like(acc)
    padded = hot.shape[0]
    if padded > bucket_count:
        G[:, :, :, :, :, bucket_count:padded] = jnp.zeros(G.shape[:-1] + (padded - bucket_count,), BF16)
    for i in range(total_steps - LAG, total_steps):
        h, t = i // steps, i % steps
        pass_on(h, t, tiles[t][1])
    spread(0, order[:AHEAD])
    late_margins = own(1)
    spread(0, order[AHEAD:])
    m_send[...] = early_margins + late_margins

    def margin_copies():
        for d in range(1, groups):
            yield pltpu.make_async_remote_copy(
                src_ref=m_send,
                dst_ref=m_recv.at[d - 1],
                send_sem=ms_sems.at[d - 1],
                recv_sem=mr_sems.at[d - 1],
                device_id={"trade": (me + d) % groups},
                device_id_type=MESH,
            )

    start(margin_copies())

    def mean_copies():
        for d in range(1, slabs):
            yield pltpu.make_async_remote_copy(
                src_ref=e_send,
                dst_ref=e_recv.at[d - 1],
                send_sem=es_sems.at[d - 1],
                recv_sem=er_sems.at[d - 1],
                device_id={"path": (slab + d) % slabs},
                device_id_type=MESH,
            )

    def margins():
        arrive(margin_copies())
        all_margins = m_send[...]
        for d in range(groups - 1):
            all_margins += m_recv[d]
        margin_o[...] = all_margins
        my_sum = jnp.sum(all_margins * pw[...], axis=1, keepdims=True)
        e_send[...] = jnp.broadcast_to(my_sum, e_send.shape)
        start(mean_copies())

    def backward(i, carry):
        h, t = i // steps, last - i % steps

        @pl.when(i == SPREAD_AT)
        def _():
            spread(1, order)

        by_width(h * steps + t, lambda h, t, width: arrive(gather2(h, t, width)))
        at = pl.multiple_of(t * TILE, TILE)

        def one(i, carry):
            part = pl.ds(pl.multiple_of(i * STEP, STEP), STEP)
            all_grad = G[h, :, :, :, :, pl.ds(at, TILE)].reshape(half_rows, TILE)
            looked_up = dot(all_grad, hot[pl.ds(at, TILE), part], NN)
            net = nets[:, part]
            total = acc[:, part]
            for n in range(half_nets):
                total += jnp.where(net == h * half_nets + n, looked_up[n * paths : (n + 1) * paths], 0.0)
            acc[:, part] = total
            return carry

        lax.fori_loop(0, capacity // STEP, one, carry, unroll=2)

        @pl.when(i == MARGINS_AT)
        def _():
            margins()

        return carry

    lax.fori_loop(0, total_steps, backward, 0)
    grad_o[...] = (acc[...] * weight[...]).astype(BF16)

    arrive(mean_copies())
    everyone = e_send[...]
    for d in range(slabs - 1):
        everyone += e_recv[d]
    expected_o[...] = everyone / (paths * slabs)

    for h in range(HALVES):
        for t, (at, width) in enumerate(tiles):
            for stage in (stage1, stage2, gather1, gather2):
                for copy in stage(h, t, width):
                    copy.wait_send()
    for copy in (*margin_copies(), *mean_copies()):
        copy.wait_send()


def finish(grad, margin, expected, grad_o, margin_o, expected_o):
    block = grad_o.shape[0]
    at = pl.multiple_of(pl.program_id(0) * block, block)
    grad_o[...] = grad[:, pl.ds(at, block)].T
    margin_o[...] = margin[...]
    net_count = margin.shape[0]
    sub = lax.broadcasted_iota(jnp.int32, margin.shape, 0)
    lane = lax.broadcasted_iota(jnp.int32, margin.shape, 1)
    row = jnp.sum(jnp.where(sub == lane, expected[...], 0.0), axis=0, keepdims=True)
    expected_o[...] = row[:, 0:net_count]


def shards(groups, slabs, deltas, net_ids, block_ids, bucket_map, risk_weight, counts, correlation, path_weight, margin_cotangent):
    capacity, paths = deltas.shape
    buckets = correlation.shape[0]
    net_count = margin_cotangent.shape[0]
    rows = net_count * paths
    half = rows // HALVES // groups // 2
    tile_count = len(tiles_of(buckets))
    padded = tile_count * TILE
    vmem = pl.BlockSpec(memory_space=pltpu.VMEM)
    smem = pl.BlockSpec(memory_space=pltpu.SMEM)
    dma = pltpu.SemaphoreType.DMA
    anywhere = pl.BlockSpec(memory_space=pltpu.HBM)
    in_hbm = functools.partial(pltpu.with_memory_space_constraint, memory_space=pltpu.HBM)
    margin, expected, turned_grad = pl.pallas_call(
        functools.partial(kernel, groups, slabs),
        out_shape=(
            jax.ShapeDtypeStruct((net_count, paths), F32),
            jax.ShapeDtypeStruct((net_count, paths), F32),
            jax.ShapeDtypeStruct((paths, capacity), BF16),
        ),
        in_specs=[anywhere] * 5 + [smem] + [anywhere] * 3,
        out_specs=(vmem, vmem, vmem),
        scratch_shapes=[
            pltpu.VMEM((capacity, paths), BF16),
            pltpu.VMEM((1, capacity), jnp.int32),
            pltpu.VMEM((1, capacity), jnp.int32),
            pltpu.VMEM((risk_weight.size // LANES, LANES), F32),
            pltpu.VMEM((bucket_map.size // LANES, LANES), jnp.int32),
            pltpu.VMEM((1, paths), F32),
            pltpu.VMEM((net_count, paths), F32),
            pltpu.VMEM((1, capacity), F32),
            pltpu.VMEM((4 * LANES, LANES), BF16),
            pltpu.VMEM((padded, capacity), BF16),
            pltpu.VMEM((rows, capacity), BF16),
            pltpu.VMEM((1, capacity), F32),
            pltpu.VMEM((HALVES, SIDE, SIDE, 2, half, padded), BF16),
            pltpu.VMEM((HALVES, 2, OTHERS, SIDE, half, buckets), BF16),
            pltpu.VMEM((HALVES, 2, SIDE, half, buckets), BF16),
            pltpu.VMEM((HALVES, 2, OTHERS, half, buckets), BF16),
            pltpu.VMEM((2 * half, buckets), F32),
            pltpu.VMEM((buckets, buckets), F32),
            pltpu.VMEM((buckets, buckets), BF16),
            pltpu.VMEM((buckets, buckets), BF16),
            pltpu.VMEM((HALVES, SIDE, SIDE, 2, half, padded), BF16),
            pltpu.VMEM((paths, capacity), F32),
            pltpu.VMEM((net_count, paths), F32),
            pltpu.VMEM((groups - 1, net_count, paths), F32),
            pltpu.VMEM((net_count, paths), F32),
            pltpu.VMEM((slabs - 1, net_count, paths), F32),
            dma,
            dma((7,)),
            dma((8, HALVES * tile_count, OTHERS)),
            dma((8, HALVES * tile_count, OTHERS)),
            dma((groups - 1,)),
            dma((groups - 1,)),
            dma((slabs - 1,)),
            dma((slabs - 1,)),
        ],
        compiler_params=pltpu.CompilerParams(
            collective_id=0, has_side_effects=True, vmem_limit_bytes=52 * 1024 * 1024
        ),
        name="margin_exchange",
    )(
        in_hbm(deltas),
        in_hbm(net_ids.reshape(1, capacity)),
        in_hbm(block_ids.reshape(1, capacity)),
        in_hbm(risk_weight.reshape(-1, LANES)),
        in_hbm(bucket_map.reshape(-1, LANES)),
        counts,
        in_hbm(correlation),
        in_hbm(path_weight.reshape(1, paths)),
        in_hbm(margin_cotangent),
    )
    block = capacity // 2
    whole = pl.BlockSpec((net_count, paths), lambda i: (0, 0))
    trade_grad, margin, expected = pl.pallas_call(
        finish,
        grid=(capacity // block,),
        out_shape=(
            jax.ShapeDtypeStruct((capacity, paths), BF16),
            jax.ShapeDtypeStruct((net_count, paths), F32),
            jax.ShapeDtypeStruct((1, net_count), F32),
        ),
        in_specs=[vmem, vmem, vmem],
        out_specs=(
            pl.BlockSpec((block, paths), lambda i: (i, 0)),
            whole,
            pl.BlockSpec((1, net_count), lambda i: (0, 0)),
        ),
        compiler_params=pltpu.CompilerParams(vmem_limit_bytes=8 * 1024 * 1024),
        name="finish",
    )(turned_grad, margin, expected)
    return margin, expected.reshape(net_count), trade_grad


def solution(mesh):
    placed = (
        P("trade", "path"),
        P("trade"),
        P("trade"),
        P(),
        P(),
        P("trade"),
        P(),
        P("path"),
        P(None, "path"),
    )
    return jax.shard_map(
        functools.partial(shards, mesh.shape["trade"], mesh.shape["path"]),
        mesh=mesh,
        in_specs=placed,
        out_specs=(P(None, "path"), P(), P("trade", "path")),
        check_vma=False,
    )
```
